32 devices in a mesh: gx: 8 (over z, y), gy: 4 (over x, core).
Axes of the slice: x: 2, y: 2, z: 4, core: 2. Of those that a mesh axis runs over, the one named last changes fastest.
Arguments:
- velocity: float32 [3, 96, 256, 256], P(None, 'gx', 'gy'), may hold values from -6 to 6
- target: float32 [3, 16384], P(None, ('gx', 'gy')), may hold values from -6 to 6
- weights: float32 [3, 6, 16384], P(None, None, ('gx', 'gy')), may hold values from 0.02 to 0.34
- corners: int32 [3, 16384], P(None, ('gx', 'gy')), may hold values from 0 to 250, as said below
- dest: int32 [16384, 1], P(('gx', 'gy')), may hold values from 0 to 7; in each aligned block of 512 rows (0 to 511, 512 to 1023, ...) at most 128 rows name the same one
Outputs:
- velocity_next: float32 [3, 96, 256, 256], P(None, 'gx', 'gy')
- marker_force: float32 [3, 16384], P(None, ('gx', 'gy'))
The draws below stay inside these ranges and needn't reach their ends.
Inputs may be any that keep to these rules, and one draw needn't show every extreme that they name: Each corner keeps its 6-cell box inside one device's block: corners[0] is at most 6, corners[1] at most 58, corners[2] at most 250. `dest`: among the markers of one device, at most 128 name the same streamwise index.
All inputs are finite; a program needn't handle non-finite values.
Results may differ from the reference program's by a relative error of at most 0.000071.
Values sent between devices are 32-bit elements; how exact they have to be, the bound alone decides.
No kernel may reach another device: no remote copies, remote signals or barrier semaphores. Data moves between devices by JAX's collectives and lax.ppermute only.
A program may use at most 128 MiB of HBM per device.

```python
import math
import jax
import jax.numpy as jnp
import numpy as np
from jax import lax

CX = 12
CY = 64
CZ = 256
MARK_DEV = 512
CAP = 128
NX = 96
NY = 256
NZ = 256
MARKERS = 16384
N_GX = 8
N_GY = 4


def draw_corners(key, part):
    upper = jnp.array([CX - 5, CY - 5, CZ - 5], jnp.int32)[:, None]
    return jax.random.randint(key, (3, MARKERS), 0, upper, dtype=jnp.int32)


def level_of(stream_key, shape, shards, smallest, largest):
    loudness, own = 1.0, jax.random.fold_in(stream_key, 6)
    for position, blocks in shards:
        heights = jnp.exp(jax.random.uniform(jax.random.fold_in(own, position), (blocks,), jnp.float32, smallest / len(shards), largest / len(shards)))
        loudness = loudness * jnp.repeat(heights, shape[position] // blocks).reshape([-1 if axis == position else 1 for axis in range(len(shape))])
    return loudness


def routed_block(key, own, number, rows, count, top, limit, lean):
    sequence = jax.random.permutation(key, count)
    packed, ordinary = shares(count, rows * top, limit, lean, True), shares(count, rows * top, limit, lean, False)
    places = jnp.arange(count)

    def named(sizes, turn):
        used = int((sizes > 0).sum())
        fixed = max(1, used // 4)
        shifted = fixed + (places - fixed + turn * (used - fixed)) % max(1, count - fixed)
        return jnp.zeros((count,), jnp.int32).at[sequence[jnp.where(places < fixed, places, shifted)]].set(jnp.asarray(sizes, jnp.int32))

    sizes = jnp.where(number % 4 == 0, named(packed, number // 4), named(ordinary, number - number // 4 - 1))
    mixed = jax.random.permutation(jax.random.fold_in(own, 3), count)
    giver, receiver = mixed[0:count // 2 * 2:2], mixed[1:count // 2 * 2:2]
    slack = jnp.minimum(sizes[giver] - 1, limit - sizes[receiver]) // 2
    slack = jnp.where((giver == sequence[0]) | (receiver == sequence[0]) | (sizes[receiver] == 0), 0, jnp.maximum(slack, 0))
    shifted = jax.random.randint(jax.random.fold_in(own, 4), (count // 2,), 0, 1 << 20) % (slack + 1)
    sizes = sizes.at[giver].add(-shifted).at[receiver].add(shifted)
    labels = jnp.searchsorted(jnp.cumsum(sizes), jnp.arange(rows * top), side="right").astype(jnp.int32)
    grid = labels.reshape(top, rows).T
    grid = grid[jax.random.permutation(jax.random.fold_in(own, 1), rows)]
    turn = jax.random.randint(jax.random.fold_in(own, 2), (rows, 1), 0, top)
    return jnp.take_along_axis(grid, (jnp.arange(top)[None, :] + turn) % top, axis=1)


def shares(amount, total, reach, slope, full):
    weights = [(1 << 20) // math.isqrt(standing ** slope) + 1 for standing in range(1, amount + 1)]
    largest = reach if full else min(reach, max(-(-total // amount), total * weights[0] // sum(weights)))
    least = 1 if total - largest >= amount - 1 else 0
    holding, spare = [largest] + [least] * (amount - 1), total - largest - least * (amount - 1)
    while spare > 0:
        movable = [i for i in range(1, amount) if holding[i] < largest] or [i for i in range(1, amount) if holding[i] < reach]
        whole, budget = sum([weights[i] for i in movable]), spare
        for i in movable:
            addition = min(reach - holding[i], max(1, budget * weights[i] // whole), spare)
            holding[i] = holding[i] + addition
            spare = spare - addition
    return np.array(holding)


def noise(rng, extent, scale, limit, shards=(), kind=jnp.bfloat16):
    gain = level_of(rng, extent, shards, -0.22, 0.18) if shards else 1.0
    values = jax.random.normal(rng, extent, jnp.float32) * scale * gain
    return jnp.minimum(jnp.maximum(values, -limit), limit).astype(kind)


def setup_inputs(seed: int = 0) -> dict:
    arg_keys = jax.random.split(jax.random.key(seed), 6)
    velocity = noise(arg_keys[0], (3, NX, NY, NZ), 1.0, 6.0, ((1, 8), (2, 4)), jnp.float32)
    target = noise(arg_keys[1], (3, MARKERS), 1.0, 6.0, ((1, 32),), jnp.float32)
    weights = jnp.clip(0.02 + 0.32 * jax.random.uniform(arg_keys[2], (3, 6, MARKERS), jnp.float32) ** level_of(arg_keys[2], (3, 6, MARKERS), ((2, 32),), -0.2, 0.2), 0.02, 0.34)
    corners = draw_corners(jax.random.fold_in(arg_keys[5], 71), 0)
    dest_keys = jax.random.split(jax.random.fold_in(arg_keys[4], 1), MARKERS // MARK_DEV)
    dest_turns = jax.random.permutation(jax.random.fold_in(arg_keys[4], 3), MARKERS // MARK_DEV)
    dest = jax.vmap(lambda own, number: routed_block(jax.random.fold_in(arg_keys[4], 2), own, number, MARK_DEV, N_GX, 1, CAP, 2))(dest_keys, dest_turns).reshape((MARKERS, 1))
    return dict(velocity=velocity, target=target, weights=weights, corners=corners, dest=dest)


diffusion = 0.4


def reference(velocity, target, weights, corners, dest):
    marker_ids = jnp.arange(MARKERS, dtype=jnp.int32)
    wall_row = (marker_ids // MARK_DEV) % N_GY
    start_x = (dest[:, 0] * CX + corners[0]).astype(jnp.int32)
    start_y = (wall_row * CY + corners[1]).astype(jnp.int32)
    start_z = corners[2].astype(jnp.int32)
    zero = jnp.zeros((), jnp.int32)

    def sample(px, py, pz, wx, wy, wz):
        box = lax.dynamic_slice(velocity, (zero, px, py, pz), (3, 6, 6, 6))
        return jnp.einsum("cabd,a,b,d->c", box, wx, wy, wz, precision=lax.Precision.HIGHEST)

    interpolated = jax.vmap(sample)(start_x, start_y, start_z, weights[0].T, weights[1].T, weights[2].T)
    marker_force = target - interpolated.T

    def add_box(index, field):
        px = start_x[index]
        py = start_y[index]
        pz = start_z[index]
        wx = weights[0, :, index]
        wy = weights[1, :, index]
        wz = weights[2, :, index]
        force = marker_force[:, index]
        box = force[:, None, None, None] * wx[None, :, None, None] * wy[None, None, :, None] * wz[None, None, None, :]
        current = lax.dynamic_slice(field, (zero, px, py, pz), (3, 6, 6, 6))
        return lax.dynamic_update_slice(field, current + box, (zero, px, py, pz))

    spread = lax.fori_loop(0, MARKERS, add_box, jnp.zeros_like(velocity))
    rhs = velocity + spread
    padded_y = jnp.pad(rhs, ((0, 0), (0, 0), (1, 1), (0, 0)))
    neighbours = padded_y[:, :, 2:] + padded_y[:, :, :-2]
    neighbours = neighbours + jnp.roll(rhs, 1, 1) + jnp.roll(rhs, -1, 1)
    neighbours = neighbours + jnp.roll(rhs, 1, 3) + jnp.roll(rhs, -1, 3)
    velocity_next = (rhs + diffusion * neighbours) / (1.0 + 6.0 * diffusion)
    return velocity_next, marker_force
```

```python
import functools

import jax
import jax.numpy as jnp
from jax import lax
from jax.experimental import pallas as pl
from jax.experimental.pallas import tpu as pltpu
from jax.sharding import PartitionSpec as P

SLOT_MIN = 12
SPAN = 6
ROWS = 24

diffusion = 0.4

f32 = jnp.float32
bf16 = jnp.bfloat16
i32 = jnp.int32
VMEM = pl.BlockSpec(memory_space=pltpu.VMEM)
NN = (((1,), (0,)), ((), ()))
NT = (((1,), (1,)), ((), ()))


def dot(a, b, dims=NN):
    return lax.dot_general(a, b, dims, preferred_element_type=f32)


def halves(x):
    high = x.astype(bf16)
    return high, (x - high.astype(f32)).astype(bf16)


def dot3(ah, al, bh, bl, dims=NN):
    return dot(ah, bh, dims) + dot(ah, bl, dims) + dot(al, bh, dims)


def thirds(x):
    high = x.astype(bf16).astype(f32)
    rest = x - high
    mid = rest.astype(bf16).astype(f32)
    return jnp.concatenate([high, mid, rest - mid], axis=0).astype(bf16)


def one_hot(position, slots):
    rows = lax.broadcasted_iota(i32, (slots, position.shape[1]), 0)
    return jnp.where(rows == position, 1.0, 0.0).astype(bf16)


def pack_kernel(capacity, chunked, span_y, dest_ref, target_ref, weights_ref, corners_ref, out_ref, pos_ref, rows_ref):
    owned = target_ref.shape[1]
    dest = dest_ref[...]
    lane = lax.broadcasted_iota(i32, (1, owned), 1)
    first = dest * (span_y * owned)
    key = first + corners_ref[1:2, :] * owned + lane
    column = jnp.transpose(jnp.broadcast_to(key, (8, owned)))[:, 0:1]
    ahead = jnp.where((column < key) & (column >= first), 1.0, 0.0)
    position = dest * capacity + jnp.sum(ahead, axis=0, keepdims=True).astype(i32)
    pos_ref[...] = position
    rows_ref[0:3, :] = target_ref[...]
    for dim in range(3):
        rows_ref[3 + 6 * dim : 9 + 6 * dim, :] = weights_ref[dim]
    rows_ref[21:24, :] = corners_ref[...].astype(f32)
    slots = out_ref.size // ROWS
    moved = dot(thirds(rows_ref[...]), one_hot(position, slots), NT)
    moved = moved[0:ROWS] + moved[ROWS : 2 * ROWS] + moved[2 * ROWS :]
    if chunked:
        for chunk in range(slots // capacity):
            out_ref[chunk] = moved[:, chunk * capacity : (chunk + 1) * capacity]
    else:
        out_ref[...] = moved


def split_kernel(velocity_ref, high_ref, low_ref):
    rows, cells_z = high_ref.shape[1:]
    for c in range(3):
        high, low = halves(velocity_ref[c].reshape(rows, cells_z))
        high_ref[c] = high
        low_ref[c] = low


def window(weights, corner, length):
    offset = lax.broadcasted_iota(i32, (length, weights.shape[1]), 0) - corner
    out = jnp.zeros(offset.shape, f32)
    for k in range(SPAN):
        out = jnp.where(offset == k, weights[k : k + 1, :], out)
    return out


def sample_kernel(
    chunked, tile, arrived_ref, high_ref, low_ref, velocity_ref,
    force_ref, wzh_ref, wzl_ref, wy_ref, fx_ref, x0_ref, x1_ref, y0_ref, y1_ref, boxh_ref, boxl_ref,
):
    _, cells_x, cells_y, cells_z = velocity_ref.shape
    slots = wy_ref.shape[1]
    capacity = arrived_ref.shape[2] if chunked else 0
    for t in range(slots // tile):
        at = slice(t * tile, (t + 1) * tile)
        if chunked:
            per = tile // capacity
            data = jnp.concatenate([arrived_ref[t * per + k] for k in range(per)], axis=1)
        else:
            data = arrived_ref[:, at]
        corner = data[21:24, :].astype(i32)
        wx = window(data[3:9], corner[0:1], cells_x)
        wy = window(data[9:15], corner[1:2], cells_y)
        wzh, wzl = halves(window(data[15:21], corner[2:3], cells_z))
        wzh_ref[:, at] = wzh
        wzl_ref[:, at] = wzl
        wy_ref[:, at] = wy
        forces = []
        for c in range(3):
            along = dot3(high_ref[c], low_ref[c], wzh, wzl)
            along = along.reshape(cells_x, cells_y, tile) * wy[None]
            sampled = jnp.sum(jnp.sum(along, axis=1) * wx, axis=0, keepdims=True)
            force = data[c : c + 1] - sampled
            fx_ref[c, :, at] = force * wx
            forces.append(force)
        forces = jnp.concatenate(forces + [jnp.zeros((5, tile), f32)], axis=0)
        if chunked:
            for k in range(per):
                force_ref[t * per + k] = forces[:, k * capacity : (k + 1) * capacity]
        else:
            force_ref[:, at] = forces
    wy = wy_ref[...]
    base = 0
    for x in (0, cells_x - 1):
        for c in range(3):
            high, low = halves(fx_ref[c, x : x + 1, :] * wy)
            boxh_ref[base : base + cells_y] = high
            boxl_ref[base : base + cells_y] = low
            base += cells_y
    pad = -(-cells_x // 16) * 16
    for y in (0, cells_y - 1):
        for c in range(3):
            rows = fx_ref[c] * wy[y : y + 1, :]
            rows = jnp.concatenate([rows, jnp.zeros((pad - cells_x, slots), f32)], axis=0)
            high, low = halves(rows)
            boxh_ref[base : base + pad] = high
            boxl_ref[base : base + pad] = low
            base += pad
    spread = dot3(boxh_ref[...], boxl_ref[...], wzh_ref[...], wzl_ref[...], NT)
    base = 0
    for x, ref in ((0, x0_ref), (cells_x - 1, x1_ref)):
        for c in range(3):
            ref[c] = velocity_ref[c, x] + spread[base : base + cells_y]
            base += cells_y
    for y, ref in ((0, y0_ref), (cells_y - 1, y1_ref)):
        for c in range(3):
            ref[c] = velocity_ref[c, :, y, :] + spread[base : base + cells_x]
            base += pad


def spread_kernel(velocity_ref, wzh_ref, wzl_ref, wy_ref, fx_ref, rhs_ref, boxh_ref, boxl_ref):
    _, cells_x, cells_y, cells_z = velocity_ref.shape
    wy = wy_ref[...]
    for c in range(3):
        for x in range(cells_x):
            high, low = halves(fx_ref[c, x : x + 1, :] * wy)
            boxh_ref[x * cells_y : (x + 1) * cells_y] = high
            boxl_ref[x * cells_y : (x + 1) * cells_y] = low
        spread = dot3(boxh_ref[...], boxl_ref[...], wzh_ref[...], wzl_ref[...], NT)
        rhs_ref[c] = velocity_ref[c] + spread.reshape(cells_x, cells_y, cells_z)


def finish_kernel(
    chunked, rhs_ref, x0_ref, x1_ref, y0_ref, y1_ref, returned_ref, pos_ref, next_hbm, force_ref, next_ref, sem,
):
    _, cells_x, cells_y, cells_z = rhs_ref.shape
    row = lax.broadcasted_iota(i32, (cells_y, cells_z), 0)
    scale = 1.0 / (1.0 + 6.0 * diffusion)
    copies = []
    for c in range(3):
        for x in range(cells_x):
            cell = rhs_ref[c, x]
            back = rhs_ref[c, x - 1] if x else x0_ref[c]
            ahead = rhs_ref[c, x + 1] if x < cells_x - 1 else x1_ref[c]
            below = jnp.where(row == 0, y0_ref[c, x : x + 1, :], pltpu.roll(cell, 1, 0))
            above = jnp.where(row == cells_y - 1, y1_ref[c, x : x + 1, :], pltpu.roll(cell, cells_y - 1, 0))
            side = pltpu.roll(cell, 1, 1) + pltpu.roll(cell, cells_z - 1, 1)
            near = (ahead + back) + (above + below) + side
            next_ref[c, x] = (cell + diffusion * near) * scale
        copy = pltpu.make_async_copy(next_ref.at[c], next_hbm.at[c], sem.at[c])
        copy.start()
        copies.append(copy)
    if chunked:
        held = jnp.concatenate([returned_ref[k] for k in range(returned_ref.shape[0])], axis=1)
    else:
        held = returned_ref[...]
    moved = dot(thirds(held), one_hot(pos_ref[...], held.shape[1]))
    moved = moved[0:8] + moved[8:16] + moved[16:24]
    force_ref[...] = moved[0:3]
    for copy in copies:
        copy.wait()


def per_device(velocity, target, weights, corners, dest):
    n_stream = lax.axis_size("gx")
    n_wall = lax.axis_size("gy")
    owned = target.shape[1]
    capacity = max(SLOT_MIN, 2 * owned // n_stream)
    slots = n_stream * capacity
    _, cells_x, cells_y, cells_z = velocity.shape
    chunked = capacity % 128 == 0
    tile = 256 if slots % 256 == 0 else 128
    shape = jax.ShapeDtypeStruct

    def exchange(packed):
        rows = packed.shape[1] if chunked else packed.shape[0]
        if chunked:
            return lax.all_to_all(packed, "gx", split_axis=0, concat_axis=0, tiled=True)
        packed = packed.reshape(rows, n_stream, capacity)
        packed = lax.all_to_all(packed, "gx", split_axis=1, concat_axis=1, tiled=True)
        return packed.reshape(rows, slots)

    def packed_shape(rows):
        return shape((n_stream, rows, capacity) if chunked else (rows, slots), f32)

    outgoing, position = pl.pallas_call(
        functools.partial(pack_kernel, capacity, chunked, cells_y),
        out_shape=(packed_shape(ROWS), shape((1, owned), i32)),
        in_specs=[VMEM] * 4,
        out_specs=(VMEM, VMEM),
        scratch_shapes=[pltpu.VMEM((ROWS, owned), f32)],
        name="pack",
    )(dest.reshape(1, owned), target, weights, corners)
    arrived = exchange(outgoing)

    block = cells_x * cells_y
    high, low = pl.pallas_call(
        split_kernel,
        out_shape=(shape((3, block, cells_z), bf16),) * 2,
        in_specs=[VMEM],
        out_specs=(VMEM, VMEM),
        name="split",
    )(velocity)

    pad = -(-cells_x // 16) * 16
    edge_rows = 6 * cells_y + 6 * pad
    face_x = shape((3, cells_y, cells_z), f32)
    face_y = shape((3, cells_x, cells_z), f32)
    force, wzh, wzl, wy, fx, x0, x1, y0, y1 = pl.pallas_call(
        functools.partial(sample_kernel, chunked, tile),
        out_shape=(
            packed_shape(8),
            shape((cells_z, slots), bf16),
            shape((cells_z, slots), bf16),
            shape((cells_y, slots), f32),
            shape((3, cells_x, slots), f32),
            face_x, face_x, face_y, face_y,
        ),
        in_specs=[VMEM] * 4,
        out_specs=(VMEM,) * 9,
        scratch_shapes=[pltpu.VMEM((edge_rows, slots), bf16)] * 2,
        name="sample",
    )(arrived, high, low, velocity)

    up_x = [(i, (i + 1) % n_stream) for i in range(n_stream)]
    down_x = [(j, i) for i, j in up_x]
    up_y = [(i, i + 1) for i in range(n_wall - 1)]
    down_y = [(j, i) for i, j in up_y]
    from_x0 = lax.ppermute(x1, "gx", up_x)
    from_x1 = lax.ppermute(x0, "gx", down_x)
    from_y0 = lax.ppermute(y1, "gy", up_y)
    from_y1 = lax.ppermute(y0, "gy", down_y)
    returned = exchange(force)

    rhs = pl.pallas_call(
        spread_kernel,
        out_shape=shape(velocity.shape, f32),
        in_specs=[VMEM] * 5,
        out_specs=VMEM,
        scratch_shapes=[pltpu.VMEM((block, slots), bf16)] * 2,
        cost_estimate=pl.CostEstimate(flops=18 * block * slots * cells_z, bytes_accessed=8 * 3 * block * cells_z, transcendentals=0),
        name="spread",
    )(velocity, wzh, wzl, wy, fx)

    return pl.pallas_call(
        functools.partial(finish_kernel, chunked),
        out_shape=(shape(velocity.shape, f32), shape((3, owned), f32)),
        in_specs=[VMEM] * 7,
        out_specs=(pl.BlockSpec(memory_space=pl.ANY), VMEM),
        scratch_shapes=[pltpu.VMEM(velocity.shape, f32), pltpu.SemaphoreType.DMA((3,))],
        name="finish",
    )(rhs, from_x0, from_x1, from_y0, from_y1, returned, position)


def solution(mesh):
    in_specs = (
        P(None, "gx", "gy", None),
        P(None, ("gx", "gy")),
        P(None, None, ("gx", "gy")),
        P(None, ("gx", "gy")),
        P(("gx", "gy"), None),
    )
    out_specs = (P(None, "gx", "gy", None), P(None, ("gx", "gy")))
    return jax.shard_map(
        per_device, mesh=mesh, in_specs=in_specs, out_specs=out_specs, check_vma=False
    )
```

```python
import functools

import jax
import jax.numpy as jnp
from jax import lax
from jax.experimental import pallas as pl
from jax.experimental.pallas import tpu as pltpu
from jax.sharding import PartitionSpec as P


SLOT_MIN = 12
SPAN = 6
ROWS = 24

diffusion = 0.4


f32 = jnp.float32
bf16 = jnp.bfloat16
i32 = jnp.int32
VMEM = pl.BlockSpec(memory_space=pltpu.VMEM)
HBM = pl.BlockSpec(memory_space=pltpu.HBM)
NN = (((1,), (0,)), ((), ()))
NT = (((1,), (1,)), ((), ()))


def dot(a, b, dims=NN):
    return lax.dot_general(a, b, dims, preferred_element_type=f32)


def halves(x):
    high = x.astype(bf16)
    return high, (x - high.astype(f32)).astype(bf16)


def dot3(ah, al, bh, bl, dims=NN):
    return dot(ah, bh, dims) + dot(ah, bl, dims) + dot(al, bh, dims)


def thirds(x):
    high = x.astype(bf16).astype(f32)
    rest = x - high
    mid = rest.astype(bf16).astype(f32)
    return jnp.concatenate([high, mid, rest - mid], axis=0).astype(bf16)


def one_hot(position, slots):
    rows = lax.broadcasted_iota(i32, (slots, position.shape[1]), 0)
    return jnp.where(rows == position, 1.0, 0.0).astype(bf16)


def pack_kernel(capacity, chunked, span_y, dest_ref, target_ref, weights_ref, corners_ref, out_ref, pos_ref, rows_ref):
    owned = target_ref.shape[1]
    dest = dest_ref[...]
    lane = lax.broadcasted_iota(i32, (1, owned), 1)
    first = dest * (span_y * owned)
    key = first + corners_ref[1:2, :] * owned + lane
    column = jnp.transpose(jnp.broadcast_to(key, (8, owned)))[:, 0:1]
    ahead = jnp.where((column < key) & (column >= first), 1.0, 0.0)
    position = dest * capacity + jnp.sum(ahead, axis=0, keepdims=True).astype(i32)
    pos_ref[...] = position
    rows_ref[0:3, :] = target_ref[...]
    for dim in range(3):
        rows_ref[3 + 6 * dim : 9 + 6 * dim, :] = weights_ref[dim]
    rows_ref[21:24, :] = corners_ref[...].astype(f32)
    slots = out_ref.size // ROWS
    moved = dot(thirds(rows_ref[...]), one_hot(position, slots), NT)
    moved = moved[0:ROWS] + moved[ROWS : 2 * ROWS] + moved[2 * ROWS :]
    if chunked:
        for chunk in range(slots // capacity):
            out_ref[chunk] = moved[:, chunk * capacity : (chunk + 1) * capacity]
    else:
        out_ref[...] = moved


def split_kernel(velocity_ref, high_ref, low_ref, x0_ref, x1_ref):
    _, cells_x, cells_y, cells_z = velocity_ref.shape
    high, low = halves(velocity_ref[0].reshape(cells_x * cells_y, cells_z))
    high_ref[0] = high
    low_ref[0] = low
    x0_ref[0] = velocity_ref[0, 0]
    x1_ref[0] = velocity_ref[0, cells_x - 1]


def window(weights, corner, length):
    offset = lax.broadcasted_iota(i32, (length, weights.shape[1]), 0) - corner
    out = jnp.zeros(offset.shape, f32)
    for k in range(SPAN):
        out = jnp.where(offset == k, weights[k : k + 1, :], out)
    return out


def tiles_of(arrived_ref, tile, slots):
    for t in range(slots // tile):
        at = slice(t * tile, (t + 1) * tile)
        if len(arrived_ref.shape) == 3:
            per = tile // arrived_ref.shape[2]
            yield at, jnp.concatenate([arrived_ref[t * per + k] for k in range(per)], axis=1)
        else:
            yield at, arrived_ref[:, at]


def sample_kernel(
    tile, arrived_ref, high_hbm, low_hbm, velocity_hbm,
    force_ref, wzh_hbm, wzl_hbm, wy_ref, fx_ref, y0_ref, y1_ref,
    high_ref, low_ref, lower_ref, upper_ref, wzh_ref, wzl_ref, boxh_ref, boxl_ref, in_sem, edge_sem, out_sem,
):
    cells_x, cells_z = y0_ref.shape[1:]
    cells_y, slots = wy_ref.shape
    loads = []
    for c in range(3):
        pair = [
            pltpu.make_async_copy(high_hbm.at[c], high_ref.at[c], in_sem.at[0, c]),
            pltpu.make_async_copy(low_hbm.at[c], low_ref.at[c], in_sem.at[1, c]),
        ]
        for load in pair:
            load.start()
        loads.append(pair)
    edges = [
        pltpu.make_async_copy(velocity_hbm.at[:, :, pl.ds(0, 8), :], lower_ref, edge_sem.at[0]),
        pltpu.make_async_copy(velocity_hbm.at[:, :, pl.ds(cells_y - 8, 8), :], upper_ref, edge_sem.at[1]),
    ]
    for load in edges:
        load.start()
    kept = []
    for at, data in tiles_of(arrived_ref, tile, slots):
        corner = data[21:24, :].astype(i32)
        wy_ref[:, at] = window(data[9:15], corner[1:2], cells_y)
        high, low = halves(window(data[15:21], corner[2:3], cells_z))
        wzh_ref[:, at] = high
        wzl_ref[:, at] = low
        kept.append((at, data[0:3], window(data[3:9], corner[0:1], cells_x)))
    stores = [
        pltpu.make_async_copy(wzh_ref, wzh_hbm, out_sem.at[0]),
        pltpu.make_async_copy(wzl_ref, wzl_hbm, out_sem.at[1]),
    ]
    for store in stores:
        store.start()
    for c in range(3):
        for load in loads[c]:
            load.wait()
        for at, target, wx in kept:
            along = dot3(high_ref[c], low_ref[c], wzh_ref[:, at], wzl_ref[:, at])
            along = along.reshape(cells_x, cells_y, tile) * wy_ref[:, at][None]
            sampled = jnp.sum(jnp.sum(along, axis=1) * wx, axis=0, keepdims=True)
            force = target[c : c + 1] - sampled
            fx_ref[c, :, at] = force * wx
            for k in range(force_ref.shape[0]):
                force_ref[k, c : c + 1, at] = force
    pad = boxh_ref.shape[0] // 6
    base = 0
    for y in (0, cells_y - 1):
        for c in range(3):
            rows = fx_ref[c] * wy_ref[y : y + 1, :]
            rows = jnp.concatenate([rows, jnp.zeros((pad - cells_x, slots), f32)], axis=0)
            high, low = halves(rows)
            boxh_ref[base : base + pad] = high
            boxl_ref[base : base + pad] = low
            base += pad
    spread = dot3(boxh_ref[...], boxl_ref[...], wzh_ref[...], wzl_ref[...], NT)
    for load in edges:
        load.wait()
    base = 0
    for y, slab_ref, ref in ((0, lower_ref, y0_ref), (7, upper_ref, y1_ref)):
        for c in range(3):
            ref[c] = slab_ref[c, :, y, :] + spread[base : base + cells_x]
            base += pad
    for store in stores:
        store.wait()


def spread_kernel(
    velocity_hbm, wzh_ref, wzl_ref, wy_ref, fx_ref, rhs_hbm, boxh_ref, boxl_ref, cell_ref, in_sem, out_sem,
):
    _, cells_x, cells_y, cells_z = velocity_hbm.shape
    loads = [pltpu.make_async_copy(velocity_hbm.at[c], cell_ref.at[c], in_sem.at[c]) for c in range(3)]
    stores = [pltpu.make_async_copy(cell_ref.at[c], rhs_hbm.at[c], out_sem.at[c]) for c in range(3)]
    for load in loads:
        load.start()
    wy = wy_ref[...]
    for c in range(3):
        for x in range(cells_x):
            high, low = halves(fx_ref[c, x : x + 1, :] * wy)
            boxh_ref[x * cells_y : (x + 1) * cells_y] = high
            boxl_ref[x * cells_y : (x + 1) * cells_y] = low
        spread = dot3(boxh_ref[...], boxl_ref[...], wzh_ref[...], wzl_ref[...], NT)
        loads[c].wait()
        cell_ref[c] = cell_ref[c] + spread.reshape(cells_x, cells_y, cells_z)
        stores[c].start()
    for store in stores:
        store.wait()


def finish_kernel(
    tile, n_stream, n_wall, chunked,
    rhs_hbm, x0_ref, x1_ref, y0_ref, y1_ref, left_ref, right_ref, given_ref, held_ref, pos_ref,
    next_hbm, force_ref, rhs_ref, next_ref, face_ref, wzh_ref, wzl_ref, boxh_ref, boxl_ref, in_sem, out_sem,
):
    _, cells_x, cells_y, cells_z = rhs_hbm.shape
    slots = given_ref.shape[2]
    loads = [pltpu.make_async_copy(rhs_hbm.at[c], rhs_ref.at[c], in_sem.at[c]) for c in range(3)]
    stores = [pltpu.make_async_copy(next_ref.at[c], next_hbm.at[c], out_sem.at[c]) for c in range(3)]
    for load in loads:
        load.start()
    here = lax.axis_index("gx")
    wall = lax.axis_index("gy")
    sides = (
        (0, left_ref, x0_ref, cells_x - SPAN, SPAN - 1, lax.rem(here + n_stream - 1, n_stream)),
        (1, right_ref, x1_ref, 0, 0, lax.rem(here + 1, n_stream)),
    )
    for side, arrived_ref, plane_ref, touching, row, owner in sides:
        for at, data in tiles_of(arrived_ref, tile, slots):
            corner = data[21:24, :].astype(i32)
            wy = window(data[9:15], corner[1:2], cells_y)
            high, low = halves(window(data[15:21], corner[2:3], cells_z))
            wzh_ref[:, at] = high
            wzl_ref[:, at] = low
            wx = jnp.where(corner[0:1] == touching, data[3 + row : 4 + row], 0.0)
            force = given_ref[owner, :, at] * wx
            for c in range(3):
                high, low = halves(force[c : c + 1] * wy)
                boxh_ref[c * cells_y : (c + 1) * cells_y, at] = high
                boxl_ref[c * cells_y : (c + 1) * cells_y, at] = low
        spread = dot3(boxh_ref[...], boxl_ref[...], wzh_ref[...], wzl_ref[...], NT)
        face_ref[side] = plane_ref[...] + spread.reshape(3, cells_y, cells_z)
    y = lax.broadcasted_iota(i32, (cells_y, cells_z), 0)
    lower = jnp.where(wall == 0, 0.0, 1.0).astype(f32)
    upper = jnp.where(wall == n_wall - 1, 0.0, 1.0).astype(f32)
    scale = 1.0 / (1.0 + 6.0 * diffusion)
    for c in range(3):
        loads[c].wait()
        for x in range(cells_x):
            cell = rhs_ref[c, x]
            back = rhs_ref[c, x - 1] if x else face_ref[0, c]
            ahead = rhs_ref[c, x + 1] if x < cells_x - 1 else face_ref[1, c]
            below = jnp.where(y == 0, y0_ref[c, x : x + 1, :] * lower, pltpu.roll(cell, 1, 0))
            above = jnp.where(y == cells_y - 1, y1_ref[c, x : x + 1, :] * upper, pltpu.roll(cell, cells_y - 1, 0))
            side = pltpu.roll(cell, 1, 1) + pltpu.roll(cell, cells_z - 1, 1)
            near = (ahead + back) + (above + below) + side
            next_ref[c, x] = (cell + diffusion * near) * scale
        stores[c].start()
    if chunked:
        capacity = slots // n_stream
        mine = pl.ds(pl.multiple_of(here * capacity, capacity), capacity)
        held = jnp.concatenate([given_ref[k, :, mine] for k in range(n_stream)], axis=1)
    else:
        held = held_ref[...]
    held = jnp.concatenate([held, jnp.zeros((5, slots), f32)], axis=0)
    moved = dot(thirds(held), one_hot(pos_ref[...], slots))
    moved = moved[0:8] + moved[8:16] + moved[16:24]
    force_ref[...] = moved[0:3]
    for store in stores:
        store.wait()


def per_device(velocity, target, weights, corners, dest):
    n_stream = lax.axis_size("gx")
    n_wall = lax.axis_size("gy")
    owned = target.shape[1]
    capacity = max(SLOT_MIN, 2 * owned // n_stream)
    slots = n_stream * capacity
    _, cells_x, cells_y, cells_z = velocity.shape
    block = cells_x * cells_y
    chunked = capacity % 128 == 0
    tile = 256 if slots % 256 == 0 else 128
    shape = jax.ShapeDtypeStruct
    sems = pltpu.SemaphoreType.DMA

    outgoing, position = pl.pallas_call(
        functools.partial(pack_kernel, capacity, chunked, cells_y),
        out_shape=(
            shape((n_stream, ROWS, capacity) if chunked else (ROWS, slots), f32),
            shape((1, owned), i32),
        ),
        in_specs=[VMEM] * 4,
        out_specs=(VMEM, VMEM),
        scratch_shapes=[pltpu.VMEM((ROWS, owned), f32)],
        name="pack",
    )(dest.reshape(1, owned), target, weights, corners)
    if chunked:
        arrived = lax.all_to_all(outgoing, "gx", split_axis=0, concat_axis=0, tiled=True)
    else:
        outgoing = outgoing.reshape(ROWS, n_stream, capacity)
        arrived = lax.all_to_all(outgoing, "gx", split_axis=1, concat_axis=1, tiled=True)
        arrived = arrived.reshape(ROWS, slots)

    high, low, x0, x1 = pl.pallas_call(
        split_kernel,
        grid=(3,),
        out_shape=(
            shape((3, block, cells_z), bf16),
            shape((3, block, cells_z), bf16),
            shape((3, cells_y, cells_z), f32),
            shape((3, cells_y, cells_z), f32),
        ),
        in_specs=[pl.BlockSpec((1, cells_x, cells_y, cells_z), lambda c: (c, 0, 0, 0))],
        out_specs=(
            pl.BlockSpec((1, block, cells_z), lambda c: (c, 0, 0)),
            pl.BlockSpec((1, block, cells_z), lambda c: (c, 0, 0)),
            pl.BlockSpec((1, cells_y, cells_z), lambda c: (c, 0, 0)),
            pl.BlockSpec((1, cells_y, cells_z), lambda c: (c, 0, 0)),
        ),
        name="split",
    )(velocity)

    up_x = [(i, (i + 1) % n_stream) for i in range(n_stream)]
    down_x = [(j, i) for i, j in up_x]
    up_y = [(i, (i + 1) % n_wall) for i in range(n_wall)]
    down_y = [(j, i) for i, j in up_y]
    from_x0 = lax.ppermute(x1, "gx", up_x)
    from_x1 = lax.ppermute(x0, "gx", down_x)
    left = lax.ppermute(arrived, "gx", up_x)
    right = lax.ppermute(arrived, "gx", down_x)

    pad = -(-cells_x // 16) * 16
    force, wzh, wzl, wy, fx, y0, y1 = pl.pallas_call(
        functools.partial(sample_kernel, tile),
        out_shape=(
            shape((n_stream, 3, slots), f32),
            shape((cells_z, slots), bf16),
            shape((cells_z, slots), bf16),
            shape((cells_y, slots), f32),
            shape((3, cells_x, slots), f32),
            shape((3, cells_x, cells_z), f32),
            shape((3, cells_x, cells_z), f32),
        ),
        in_specs=[VMEM, HBM, HBM, HBM],
        out_specs=(VMEM, HBM, HBM, VMEM, VMEM, VMEM, VMEM),
        scratch_shapes=[
            pltpu.VMEM((3, block, cells_z), bf16),
            pltpu.VMEM((3, block, cells_z), bf16),
            pltpu.VMEM((3, cells_x, 8, cells_z), f32),
            pltpu.VMEM((3, cells_x, 8, cells_z), f32),
            pltpu.VMEM((cells_z, slots), bf16),
            pltpu.VMEM((cells_z, slots), bf16),
            pltpu.VMEM((6 * pad, slots), bf16),
            pltpu.VMEM((6 * pad, slots), bf16),
            sems((2, 3)),
            sems((2,)),
            sems((2,)),
        ],
        compiler_params=pltpu.CompilerParams(vmem_limit_bytes=63_280_000),
        name="sample",
    )(arrived, high, low, velocity)

    from_y0 = lax.ppermute(y1, "gy", up_y)
    from_y1 = lax.ppermute(y0, "gy", down_y)
    given = lax.all_to_all(force, "gx", split_axis=0, concat_axis=0, tiled=True)
    if chunked:
        held = jnp.zeros((8, 128), f32)
    else:
        held = lax.dynamic_slice_in_dim(given, lax.axis_index("gx") * capacity, capacity, axis=2)
        held = held.transpose(1, 0, 2).reshape(3, slots)

    rhs = pl.pallas_call(
        spread_kernel,
        out_shape=shape(velocity.shape, f32),
        in_specs=[HBM, VMEM, VMEM, VMEM, VMEM],
        out_specs=HBM,
        scratch_shapes=[
            pltpu.VMEM((block, slots), bf16),
            pltpu.VMEM((block, slots), bf16),
            pltpu.VMEM(velocity.shape, f32),
            sems((3,)),
            sems((3,)),
        ],
        cost_estimate=pl.CostEstimate(flops=18 * block * slots * cells_z, bytes_accessed=24 * block * cells_z, transcendentals=0),
        name="spread",
    )(velocity, wzh, wzl, wy, fx)

    return pl.pallas_call(
        functools.partial(finish_kernel, tile, n_stream, n_wall, chunked),
        out_shape=(shape(velocity.shape, f32), shape((3, owned), f32)),
        in_specs=[HBM] + [VMEM] * 9,
        out_specs=(HBM, VMEM),
        scratch_shapes=[
            pltpu.VMEM(velocity.shape, f32),
            pltpu.VMEM(velocity.shape, f32),
            pltpu.VMEM((2, 3, cells_y, cells_z), f32),
            pltpu.VMEM((cells_z, slots), bf16),
            pltpu.VMEM((cells_z, slots), bf16),
            pltpu.VMEM((3 * cells_y, slots), bf16),
            pltpu.VMEM((3 * cells_y, slots), bf16),
            sems((3,)),
            sems((3,)),
        ],
        compiler_params=pltpu.CompilerParams(vmem_limit_bytes=62_400_000),
        name="finish",
    )(rhs, from_x0, from_x1, from_y0, from_y1, left, right, given, held, position)


def solution(mesh):
    in_specs = (
        P(None, "gx", "gy", None),
        P(None, ("gx", "gy")),
        P(None, None, ("gx", "gy")),
        P(None, ("gx", "gy")),
        P(("gx", "gy"), None),
    )
    out_specs = (P(None, "gx", "gy", None), P(None, ("gx", "gy")))
    return jax.shard_map(
        per_device, mesh=mesh, in_specs=in_specs, out_specs=out_specs, check_vma=False
    )
```

```python
import functools

import jax
import jax.numpy as jnp
from jax import lax
from jax.experimental import pallas as pl
from jax.experimental.pallas import tpu as pltpu
from jax.sharding import PartitionSpec as P


SLOT_MIN = 12
SPAN = 6
ROWS = 24

diffusion = 0.4


f32 = jnp.float32
bf16 = jnp.bfloat16
i32 = jnp.int32
VMEM = pl.BlockSpec(memory_space=pltpu.VMEM)
HBM = pl.BlockSpec(memory_space=pltpu.HBM)
NN = (((1,), (0,)), ((), ()))
NT = (((1,), (1,)), ((), ()))


def dot(a, b, dims=NN):
    return lax.dot_general(a, b, dims, preferred_element_type=f32)


def halves(x):
    high = x.astype(bf16)
    return high, (x - high.astype(f32)).astype(bf16)


def dot3(ah, al, bh, bl, dims=NN):
    return dot(ah, bh, dims) + dot(ah, bl, dims) + dot(al, bh, dims)


def thirds(x):
    high = x.astype(bf16).astype(f32)
    rest = x - high
    mid = rest.astype(bf16).astype(f32)
    return jnp.concatenate([high, mid, rest - mid], axis=0).astype(bf16)


def one_hot(position, first, slots):
    rows = lax.broadcasted_iota(i32, (slots, position.shape[1]), 0) + first
    return jnp.where(rows == position, 1.0, 0.0).astype(bf16)


def span(index, size):
    return pl.ds(pl.multiple_of(index * size, size), size)


def loop(count, body):
    def step(index, _):
        body(index)

    lax.fori_loop(0, count, step, None)


def pack_kernel(
    capacity, tile, span_y, dest_ref, target_ref, weights_ref, corners_ref, out_ref, pos_ref, rows_ref, column_ref,
):
    owned = target_ref.shape[1]
    dest = dest_ref[...]
    lane = lax.broadcasted_iota(i32, (1, owned), 1)
    first = dest * (span_y * owned)
    key = first + corners_ref[1:2, :] * owned + lane
    column_ref[...] = jnp.transpose(jnp.broadcast_to(key, (8, owned)))

    def count(index, total):
        column = column_ref[span(index, 64), 0:1]
        ahead = jnp.where((column < key) & (column >= first), 1.0, 0.0)
        return total + jnp.sum(ahead, axis=0, keepdims=True)

    rank = lax.fori_loop(0, owned // 64, count, jnp.zeros((1, owned), f32))
    position = dest * capacity + rank.astype(i32)
    pos_ref[...] = position
    rows_ref[0:3, :] = target_ref[...]
    for dim in range(3):
        rows_ref[3 + 6 * dim : 9 + 6 * dim, :] = weights_ref[dim]
    rows_ref[21:24, :] = corners_ref[...].astype(f32)
    data = thirds(rows_ref[...])
    chunked = len(out_ref.shape) == 3

    def move(t):
        moved = dot(data, one_hot(position, t * tile, tile), NT)
        moved = moved[0:ROWS] + moved[ROWS : 2 * ROWS] + moved[2 * ROWS :]
        if chunked:
            per = tile // capacity
            for k in range(per):
                out_ref[t * per + k] = moved[:, k * capacity : (k + 1) * capacity]
        else:
            out_ref[:, span(t, tile)] = moved

    loop(out_ref.size // ROWS // tile, move)


def split_kernel(velocity_ref, high_ref, low_ref, x0_ref, x1_ref):
    _, cells_x, cells_y, cells_z = velocity_ref.shape
    high, low = halves(velocity_ref[0].reshape(cells_x * cells_y, cells_z))
    high_ref[0] = high
    low_ref[0] = low
    x0_ref[0] = velocity_ref[0, 0]
    x1_ref[0] = velocity_ref[0, cells_x - 1]


def window(weights, corner, length):
    offset = lax.broadcasted_iota(i32, (length, weights.shape[1]), 0) - corner
    out = jnp.zeros(offset.shape, f32)
    for k in range(SPAN):
        out = jnp.where(offset == k, weights[k : k + 1, :], out)
    return out


def markers(arrived_ref, t, tile):
    if len(arrived_ref.shape) == 3:
        per = tile // arrived_ref.shape[2]
        return jnp.concatenate([arrived_ref[t * per + k] for k in range(per)], axis=1)
    return arrived_ref[:, span(t, tile)]


def sample_kernel(
    tile, cells_x, arrived_ref, high_hbm, low_hbm, velocity_hbm,
    force_ref, wzh_hbm, wzl_hbm, wy_ref, fx_ref, y0_ref, y1_ref,
    high_ref, low_ref, lower_ref, upper_ref, wzh_ref, wzl_ref, wx_ref, goal_ref, face_ref, in_sem, edge_sem, out_sem,
):
    cells_z = y0_ref.shape[2]
    cells_y, slots = wy_ref.shape
    pad = wx_ref.shape[0]
    count = slots // tile
    loads = [
        pltpu.make_async_copy(high_hbm, high_ref, in_sem.at[0]),
        pltpu.make_async_copy(low_hbm, low_ref, in_sem.at[1]),
        pltpu.make_async_copy(velocity_hbm.at[:, :, pl.ds(0, 8), :], lower_ref, edge_sem.at[0]),
        pltpu.make_async_copy(velocity_hbm.at[:, :, pl.ds(cells_y - 8, 8), :], upper_ref, edge_sem.at[1]),
    ]
    for load in loads:
        load.start()

    def windows(t):
        at = span(t, tile)
        data = markers(arrived_ref, t, tile)
        corner = data[21:24, :].astype(i32)
        for c in range(3):
            goal_ref[c, 0:1, at] = data[c : c + 1]
        wx_ref[:, at] = window(data[3:9], corner[0:1], pad)
        wy_ref[:, at] = window(data[9:15], corner[1:2], cells_y)
        high, low = halves(window(data[15:21], corner[2:3], cells_z))
        wzh_ref[:, at] = high
        wzl_ref[:, at] = low

    loop(count, windows)
    stores = [
        pltpu.make_async_copy(wzh_ref, wzh_hbm, out_sem.at[0]),
        pltpu.make_async_copy(wzl_ref, wzl_hbm, out_sem.at[1]),
    ]
    for store in stores:
        store.start()
    for load in loads:
        load.wait()

    def sample(index):
        c, t = lax.div(index, count), lax.rem(index, count)
        at = span(t, tile)
        along = dot3(high_ref[c], low_ref[c], wzh_ref[:, at], wzl_ref[:, at])
        along = along.reshape(cells_x, cells_y, tile) * wy_ref[:, at][None]
        wx = wx_ref[:, at]
        sampled = jnp.sum(jnp.sum(along, axis=1) * wx[0:cells_x], axis=0, keepdims=True)
        force = goal_ref[c, 0:1, at] - sampled
        fx_ref[c, :, at] = force * wx
        goal_ref[c, 0:1, at] = force

    loop(3 * count, sample)

    def give(k):
        for c in range(3):
            force_ref[k, c : c + 1, :] = goal_ref[c, 0:1, :]

    loop(force_ref.shape[0], give)
    face_ref[...] = jnp.zeros_like(face_ref)

    def edges(t):
        at = span(t, tile)
        wy = wy_ref[:, at]
        rows = [fx_ref[c, :, at] * wy[y : y + 1] for y in (0, cells_y - 1) for c in range(3)]
        high, low = halves(jnp.concatenate(rows, axis=0))
        face_ref[...] += dot3(high, low, wzh_ref[:, at], wzl_ref[:, at], NT)

    loop(count, edges)
    base = 0
    for y, slab_ref, ref in ((0, lower_ref, y0_ref), (7, upper_ref, y1_ref)):
        for c in range(3):
            ref[c] = slab_ref[c, :, y, :] + face_ref[base : base + cells_x]
            base += pad
    for store in stores:
        store.wait()


def spread_kernel(
    tile, velocity_hbm, wzh_ref, wzl_ref, wy_ref, fx_ref, rhs_hbm, boxh_ref, boxl_ref, cell_ref, in_sem, out_sem,
):
    _, cells_x, cells_y, cells_z = velocity_hbm.shape
    count = wy_ref.shape[1] // tile
    load = pltpu.make_async_copy(velocity_hbm, cell_ref, in_sem)
    load.start()
    load.wait()

    def store(c):
        return pltpu.make_async_copy(cell_ref.at[c], rhs_hbm.at[c], out_sem.at[c])

    def spread(index):
        c, t = lax.div(index, count), lax.rem(index, count)
        at = span(t, tile)
        wy = wy_ref[:, at]
        for x in range(cells_x):
            high, low = halves(fx_ref[c, x : x + 1, at] * wy)
            boxh_ref[x * cells_y : (x + 1) * cells_y] = high
            boxl_ref[x * cells_y : (x + 1) * cells_y] = low
        added = dot3(boxh_ref[...], boxl_ref[...], wzh_ref[:, at], wzl_ref[:, at], NT)
        cell_ref[c] += added.reshape(cells_x, cells_y, cells_z)

        @pl.when(t == count - 1)
        def _():
            store(c).start()

    loop(3 * count, spread)
    for c in range(3):
        store(c).wait()


def finish_kernel(
    tile, n_stream, n_wall, chunked,
    rhs_hbm, x0_ref, x1_ref, y0_ref, y1_ref, left_ref, right_ref, given_ref, held_ref, pos_ref,
    next_hbm, force_ref, rhs_ref, next_ref, moved_ref, in_sem, out_sem,
):
    _, cells_x, cells_y, cells_z = rhs_hbm.shape
    slots = given_ref.shape[2]
    count = slots // tile
    loads = [
        pltpu.make_async_copy(rhs_hbm.at[c], rhs_ref.at[c, pl.ds(1, cells_x)], in_sem.at[c]) for c in range(3)
    ]
    for load in loads:
        load.start()
    here = lax.axis_index("gx")
    wall = lax.axis_index("gy")
    for c in range(3):
        rhs_ref[c, 0] = x0_ref[c]
        rhs_ref[c, cells_x + 1] = x1_ref[c]
    before = lax.rem(here + n_stream - 1, n_stream)
    after = lax.rem(here + 1, n_stream)

    def edges(index):
        side, t = lax.div(index, count), lax.rem(index, count)
        at = span(t, tile)
        first = side == 0
        data = jnp.where(first, markers(left_ref, t, tile), markers(right_ref, t, tile))
        corner = data[21:24, :].astype(i32)
        wy = window(data[9:15], corner[1:2], cells_y)
        wzh, wzl = halves(window(data[15:21], corner[2:3], cells_z))
        wx = jnp.where(first, data[8:9], data[3:4])
        wx = jnp.where(corner[0:1] == jnp.where(first, cells_x - SPAN, 0), wx, 0.0)
        force = given_ref[jnp.where(first, before, after), :, at] * wx
        high, low = halves(jnp.concatenate([force[c : c + 1] * wy for c in range(3)], axis=0))
        added = dot3(high, low, wzh, wzl, NT)
        plane = side * (cells_x + 1)
        for c in range(3):
            rhs_ref[c, plane] += added[c * cells_y : (c + 1) * cells_y]

    loop(2 * count, edges)
    y = lax.broadcasted_iota(i32, (cells_y, cells_z), 0)
    lower = jnp.where(wall == 0, 0.0, 1.0).astype(f32)
    upper = jnp.where(wall == n_wall - 1, 0.0, 1.0).astype(f32)
    scale = 1.0 / (1.0 + 6.0 * diffusion)
    for load in loads:
        load.wait()

    def store(c):
        return pltpu.make_async_copy(next_ref.at[c], next_hbm.at[c], out_sem.at[c])

    def stencil(index):
        c, x = lax.div(index, cells_x), lax.rem(index, cells_x)
        cell = rhs_ref[c, x + 1]
        below = jnp.where(y == 0, y0_ref[c, pl.ds(x, 1), :] * lower, pltpu.roll(cell, 1, 0))
        above = jnp.where(y == cells_y - 1, y1_ref[c, pl.ds(x, 1), :] * upper, pltpu.roll(cell, cells_y - 1, 0))
        side = pltpu.roll(cell, 1, 1) + pltpu.roll(cell, cells_z - 1, 1)
        near = (rhs_ref[c, x + 2] + rhs_ref[c, x]) + (above + below) + side
        next_ref[c, x] = (cell + diffusion * near) * scale

        @pl.when(x == cells_x - 1)
        def _():
            store(c).start()

    loop(3 * cells_x, stencil)
    moved_ref[...] = jnp.zeros_like(moved_ref)
    position = pos_ref[...]

    def unpack(t):
        if chunked:
            capacity = slots // n_stream
            per = tile // capacity
            mine = span(here, capacity)
            held = jnp.concatenate([given_ref[t * per + k, :, mine] for k in range(per)], axis=1)
        else:
            held = held_ref[:, span(t, tile)]
        held = jnp.concatenate([held, jnp.zeros((5, tile), f32)], axis=0)
        moved_ref[...] += dot(thirds(held), one_hot(position, t * tile, tile))

    loop(count, unpack)
    force_ref[...] = (moved_ref[0:8] + moved_ref[8:16] + moved_ref[16:24])[0:3]
    for c in range(3):
        store(c).wait()


def per_device(velocity, target, weights, corners, dest):
    n_stream = lax.axis_size("gx")
    n_wall = lax.axis_size("gy")
    owned = target.shape[1]
    capacity = max(SLOT_MIN, 2 * owned // n_stream)
    slots = n_stream * capacity
    _, cells_x, cells_y, cells_z = velocity.shape
    block = cells_x * cells_y
    chunked = capacity % 128 == 0
    tile = 256 if slots % 256 == 0 else 128
    shape = jax.ShapeDtypeStruct
    sems = pltpu.SemaphoreType.DMA

    outgoing, position = pl.pallas_call(
        functools.partial(pack_kernel, capacity, tile, cells_y),
        out_shape=(
            shape((n_stream, ROWS, capacity) if chunked else (ROWS, slots), f32),
            shape((1, owned), i32),
        ),
        in_specs=[VMEM] * 4,
        out_specs=(VMEM, VMEM),
        scratch_shapes=[pltpu.VMEM((ROWS, owned), f32), pltpu.VMEM((owned, 8), i32)],
        name="pack",
    )(dest.reshape(1, owned), target, weights, corners)
    if chunked:
        arrived = lax.all_to_all(outgoing, "gx", split_axis=0, concat_axis=0, tiled=True)
    else:
        outgoing = outgoing.reshape(ROWS, n_stream, capacity)
        arrived = lax.all_to_all(outgoing, "gx", split_axis=1, concat_axis=1, tiled=True)
        arrived = arrived.reshape(ROWS, slots)

    high, low, x0, x1 = pl.pallas_call(
        split_kernel,
        grid=(3,),
        out_shape=(
            shape((3, block, cells_z), bf16),
            shape((3, block, cells_z), bf16),
            shape((3, cells_y, cells_z), f32),
            shape((3, cells_y, cells_z), f32),
        ),
        in_specs=[pl.BlockSpec((1, cells_x, cells_y, cells_z), lambda c: (c, 0, 0, 0))],
        out_specs=(
            pl.BlockSpec((1, block, cells_z), lambda c: (c, 0, 0)),
            pl.BlockSpec((1, block, cells_z), lambda c: (c, 0, 0)),
            pl.BlockSpec((1, cells_y, cells_z), lambda c: (c, 0, 0)),
            pl.BlockSpec((1, cells_y, cells_z), lambda c: (c, 0, 0)),
        ),
        name="split",
    )(velocity)

    up_x = [(i, (i + 1) % n_stream) for i in range(n_stream)]
    down_x = [(j, i) for i, j in up_x]
    up_y = [(i, (i + 1) % n_wall) for i in range(n_wall)]
    down_y = [(j, i) for i, j in up_y]
    from_x0 = lax.ppermute(x1, "gx", up_x)
    from_x1 = lax.ppermute(x0, "gx", down_x)
    left = lax.ppermute(arrived, "gx", up_x)
    right = lax.ppermute(arrived, "gx", down_x)

    pad = -(-cells_x // 16) * 16
    force, wzh, wzl, wy, fx, y0, y1 = pl.pallas_call(
        functools.partial(sample_kernel, tile, cells_x),
        out_shape=(
            shape((n_stream, 3, slots), f32),
            shape((cells_z, slots), bf16),
            shape((cells_z, slots), bf16),
            shape((cells_y, slots), f32),
            shape((3, pad, slots), f32),
            shape((3, cells_x, cells_z), f32),
            shape((3, cells_x, cells_z), f32),
        ),
        in_specs=[VMEM, HBM, HBM, HBM],
        out_specs=(VMEM, HBM, HBM, VMEM, VMEM, VMEM, VMEM),
        scratch_shapes=[
            pltpu.VMEM((3, block, cells_z), bf16),
            pltpu.VMEM((3, block, cells_z), bf16),
            pltpu.VMEM((3, cells_x, 8, cells_z), f32),
            pltpu.VMEM((3, cells_x, 8, cells_z), f32),
            pltpu.VMEM((cells_z, slots), bf16),
            pltpu.VMEM((cells_z, slots), bf16),
            pltpu.VMEM((pad, slots), f32),
            pltpu.VMEM((3, 8, slots), f32),
            pltpu.VMEM((6 * pad, cells_z), f32),
            sems((2,)),
            sems((2,)),
            sems((2,)),
        ],
        compiler_params=pltpu.CompilerParams(vmem_limit_bytes=63_280_000),
        name="sample",
    )(arrived, high, low, velocity)

    from_y0 = lax.ppermute(y1, "gy", up_y)
    from_y1 = lax.ppermute(y0, "gy", down_y)
    given = lax.all_to_all(force, "gx", split_axis=0, concat_axis=0, tiled=True)
    if chunked:
        held = position
    else:
        held = lax.dynamic_slice_in_dim(given, lax.axis_index("gx") * capacity, capacity, axis=2)
        held = held.transpose(1, 0, 2).reshape(3, slots)

    rhs = pl.pallas_call(
        functools.partial(spread_kernel, tile),
        out_shape=shape(velocity.shape, f32),
        in_specs=[HBM, VMEM, VMEM, VMEM, VMEM],
        out_specs=HBM,
        scratch_shapes=[
            pltpu.VMEM((block, tile), bf16),
            pltpu.VMEM((block, tile), bf16),
            pltpu.VMEM(velocity.shape, f32),
            sems(()),
            sems((3,)),
        ],
        cost_estimate=pl.CostEstimate(flops=18 * block * slots * cells_z, bytes_accessed=24 * block * cells_z, transcendentals=0),
        name="spread",
    )(velocity, wzh, wzl, wy, fx)

    return pl.pallas_call(
        functools.partial(finish_kernel, tile, n_stream, n_wall, chunked),
        out_shape=(shape(velocity.shape, f32), shape((3, owned), f32)),
        in_specs=[HBM] + [VMEM] * 9,
        out_specs=(HBM, VMEM),
        scratch_shapes=[
            pltpu.VMEM((3, cells_x + 2, cells_y, cells_z), f32),
            pltpu.VMEM(velocity.shape, f32),
            pltpu.VMEM((24, owned), f32),
            sems((3,)),
            sems((3,)),
        ],
        compiler_params=pltpu.CompilerParams(vmem_limit_bytes=62_400_000),
        name="finish",
    )(rhs, from_x0, from_x1, from_y0, from_y1, left, right, given, held, position)


def solution(mesh):
    in_specs = (
        P(None, "gx", "gy", None),
        P(None, ("gx", "gy")),
        P(None, None, ("gx", "gy")),
        P(None, ("gx", "gy")),
        P(("gx", "gy"), None),
    )
    out_specs = (P(None, "gx", "gy", None), P(None, ("gx", "gy")))
    return jax.shard_map(
        per_device, mesh=mesh, in_specs=in_specs, out_specs=out_specs, check_vma=False
    )
```

```python
import functools

import jax
import jax.numpy as jnp
from jax import lax
from jax.experimental import pallas as pl
from jax.experimental.pallas import tpu as pltpu
from jax.sharding import PartitionSpec as P


SLOT_MIN = 12
SPAN = 6
ROWS = 24

diffusion = 0.4


f32 = jnp.float32
bf16 = jnp.bfloat16
i32 = jnp.int32
VMEM = pl.BlockSpec(memory_space=pltpu.VMEM)
HBM = pl.BlockSpec(memory_space=pltpu.HBM)
NN = (((1,), (0,)), ((), ()))
NT = (((1,), (1,)), ((), ()))


def dot(a, b, dims=NN):
    return lax.dot_general(a, b, dims, preferred_element_type=f32)


def halves(x):
    high = x.astype(bf16)
    return high, (x - high.astype(f32)).astype(bf16)


def dot3(ah, al, bh, bl, dims=NN):
    return dot(ah, bh, dims) + dot(ah, bl, dims) + dot(al, bh, dims)


def thirds(x):
    high = x.astype(bf16).astype(f32)
    rest = x - high
    mid = rest.astype(bf16).astype(f32)
    return jnp.concatenate([high, mid, rest - mid], axis=0).astype(bf16)


def one_hot(position, slots):
    rows = lax.broadcasted_iota(i32, (slots, position.shape[1]), 0)
    return jnp.where(rows == position, 1.0, 0.0).astype(bf16)


def span(index, size):
    return pl.ds(pl.multiple_of(index * size, size), size)


def pack_kernel(
    capacity, chunked, dest_ref, target_ref, weights_ref, corners_ref, velocity_hbm,
    out_ref, pos_ref, x0_hbm, x1_hbm, rows_ref, sem,
):
    owned = target_ref.shape[1]
    cells_x = velocity_hbm.shape[1]
    faces = [
        pltpu.make_async_copy(velocity_hbm.at[:, 0], x0_hbm, sem.at[0]),
        pltpu.make_async_copy(velocity_hbm.at[:, cells_x - 1], x1_hbm, sem.at[1]),
    ]
    for face in faces:
        face.start()
    dest = dest_ref[...]
    corner = corners_ref[0:1, :]
    lane = lax.broadcasted_iota(i32, (1, owned), 1)
    last = corner == cells_x - SPAN
    group = jnp.where(last, 2, jnp.where(corner == 0, 0, 1))
    first = (dest * 4 + jnp.where(last, 2, 0)) * owned
    key = (dest * 4 + group) * owned + lane
    column = jnp.transpose(jnp.broadcast_to(key, (8, owned)))[:, 0:1]
    ahead = jnp.where((column < key) & (column >= first), 1.0, 0.0)
    rank = jnp.sum(ahead, axis=0, keepdims=True).astype(i32)
    position = dest * capacity + jnp.where(last, capacity - 1 - rank, rank)
    pos_ref[...] = position
    rows_ref[0:3, :] = target_ref[...]
    for dim in range(3):
        rows_ref[3 + 6 * dim : 9 + 6 * dim, :] = weights_ref[dim]
    rows_ref[21:24, :] = corners_ref[...].astype(f32)
    slots = out_ref.size // ROWS
    moved = dot(thirds(rows_ref[...]), one_hot(position, slots), NT)
    moved = moved[0:ROWS] + moved[ROWS : 2 * ROWS] + moved[2 * ROWS :]
    if chunked:
        for chunk in range(slots // capacity):
            out_ref[chunk] = moved[:, chunk * capacity : (chunk + 1) * capacity]
    else:
        out_ref[...] = moved
    for face in faces:
        face.wait()


def split_kernel(velocity_ref, high_ref, low_ref):
    _, cells_x, cells_y, cells_z = velocity_ref.shape
    high, low = halves(velocity_ref[0].reshape(cells_x * cells_y, cells_z))
    high_ref[0] = high
    low_ref[0] = low


def window(weights, corner, length):
    offset = lax.broadcasted_iota(i32, (length, weights.shape[1]), 0) - corner
    out = jnp.zeros(offset.shape, f32)
    for k in range(SPAN):
        out = jnp.where(offset == k, weights[k : k + 1, :], out)
    return out


def tiles_of(arrived_ref, tile, slots):
    for t in range(slots // tile):
        at = slice(t * tile, (t + 1) * tile)
        if len(arrived_ref.shape) == 3:
            per = tile // arrived_ref.shape[2]
            yield at, jnp.concatenate([arrived_ref[t * per + k] for k in range(per)], axis=1)
        else:
            yield at, arrived_ref[:, at]


def sample_kernel(
    tile, arrived_ref, high_hbm, low_hbm, velocity_hbm,
    force_ref, wzh_hbm, wzl_hbm, wy_ref, fx_ref, y0_ref, y1_ref,
    high_ref, low_ref, lower_ref, upper_ref, wzh_ref, wzl_ref, boxh_ref, boxl_ref, in_sem, edge_sem, out_sem,
):
    cells_x, cells_z = y0_ref.shape[1:]
    cells_y, slots = wy_ref.shape
    loads = []
    for c in range(3):
        pair = [
            pltpu.make_async_copy(high_hbm.at[c], high_ref.at[c], in_sem.at[0, c]),
            pltpu.make_async_copy(low_hbm.at[c], low_ref.at[c], in_sem.at[1, c]),
        ]
        for load in pair:
            load.start()
        loads.append(pair)
    edges = [
        pltpu.make_async_copy(velocity_hbm.at[:, :, pl.ds(0, 8), :], lower_ref, edge_sem.at[0]),
        pltpu.make_async_copy(velocity_hbm.at[:, :, pl.ds(cells_y - 8, 8), :], upper_ref, edge_sem.at[1]),
    ]
    for load in edges:
        load.start()
    kept = []
    for at, data in tiles_of(arrived_ref, tile, slots):
        corner = data[21:24, :].astype(i32)
        wy_ref[:, at] = window(data[9:15], corner[1:2], cells_y)
        high, low = halves(window(data[15:21], corner[2:3], cells_z))
        wzh_ref[:, at] = high
        wzl_ref[:, at] = low
        kept.append((at, data[0:3], window(data[3:9], corner[0:1], cells_x)))
    stores = [
        pltpu.make_async_copy(wzh_ref, wzh_hbm, out_sem.at[0]),
        pltpu.make_async_copy(wzl_ref, wzl_hbm, out_sem.at[1]),
    ]
    for store in stores:
        store.start()
    for c in range(3):
        for load in loads[c]:
            load.wait()
        for at, target, wx in kept:
            along = dot3(high_ref[c], low_ref[c], wzh_ref[:, at], wzl_ref[:, at])
            along = along.reshape(cells_x, cells_y, tile) * wy_ref[:, at][None]
            sampled = jnp.sum(jnp.sum(along, axis=1) * wx, axis=0, keepdims=True)
            force = target[c : c + 1] - sampled
            fx_ref[c, :, at] = force * wx
            for k in range(force_ref.shape[0]):
                force_ref[k, c : c + 1, at] = force
    pad = boxh_ref.shape[0] // 6
    base = 0
    for y in (0, cells_y - 1):
        for c in range(3):
            rows = fx_ref[c] * wy_ref[y : y + 1, :]
            rows = jnp.concatenate([rows, jnp.zeros((pad - cells_x, slots), f32)], axis=0)
            high, low = halves(rows)
            boxh_ref[base : base + pad] = high
            boxl_ref[base : base + pad] = low
            base += pad
    spread = dot3(boxh_ref[...], boxl_ref[...], wzh_ref[...], wzl_ref[...], NT)
    for load in edges:
        load.wait()
    base = 0
    for y, slab_ref, ref in ((0, lower_ref, y0_ref), (7, upper_ref, y1_ref)):
        for c in range(3):
            ref[c] = slab_ref[c, :, y, :] + spread[base : base + cells_x]
            base += pad
    for store in stores:
        store.wait()


def spread_kernel(
    velocity_hbm, wzh_ref, wzl_ref, wy_ref, fx_ref, rhs_hbm, boxh_ref, boxl_ref, cell_ref, in_sem, out_sem,
):
    _, cells_x, cells_y, cells_z = velocity_hbm.shape
    loads = [pltpu.make_async_copy(velocity_hbm.at[c], cell_ref.at[c], in_sem.at[c]) for c in range(3)]
    stores = [pltpu.make_async_copy(cell_ref.at[c], rhs_hbm.at[c], out_sem.at[c]) for c in range(3)]
    for load in loads:
        load.start()
    wy = wy_ref[...]
    for c in range(3):
        for x in range(cells_x):
            high, low = halves(fx_ref[c, x : x + 1, :] * wy)
            boxh_ref[x * cells_y : (x + 1) * cells_y] = high
            boxl_ref[x * cells_y : (x + 1) * cells_y] = low
        spread = dot3(boxh_ref[...], boxl_ref[...], wzh_ref[...], wzl_ref[...], NT)
        loads[c].wait()
        cell_ref[c] = cell_ref[c] + spread.reshape(cells_x, cells_y, cells_z)
        stores[c].start()
    for store in stores:
        store.wait()


def quarter(marks_ref, side, index, width):
    lane = lax.broadcasted_iota(i32, marks_ref.shape[2:], 1)
    capacity = marks_ref.shape[3]
    per = capacity // width
    out = []
    for base in range(0, marks_ref.shape[1], per):
        piece = jnp.zeros(marks_ref.shape[2:], f32)
        for k in range(per):
            moved = pltpu.roll(marks_ref[side, base + k], lax.rem(capacity + (k - index) * width, capacity), 1)
            piece = jnp.where((lane >= k * width) & (lane < (k + 1) * width), moved, piece)
        out.append(piece)
    return jnp.concatenate(out, axis=1)


def finish_kernel(
    tile, n_stream, n_wall, chunked, quartered,
    rhs_hbm, x0_ref, x1_ref, y0_ref, y1_ref, left_ref, right_ref, given_ref, held_ref, pos_ref,
    next_hbm, force_ref, rhs_ref, next_ref, face_ref, marks_ref, in_sem, out_sem,
):
    _, cells_x, cells_y, cells_z = rhs_hbm.shape
    slots = given_ref.shape[2]
    loads = [pltpu.make_async_copy(rhs_hbm.at[c], rhs_ref.at[c], in_sem.at[c]) for c in range(3)]
    stores = [pltpu.make_async_copy(next_ref.at[c], next_hbm.at[c], out_sem.at[c]) for c in range(3)]
    for load in loads:
        load.start()
    here = lax.axis_index("gx")
    wall = lax.axis_index("gy")
    sides = (
        (0, left_ref, x0_ref, cells_x - SPAN, SPAN - 1, lax.rem(here + n_stream - 1, n_stream)),
        (1, right_ref, x1_ref, 0, 0, lax.rem(here + 1, n_stream)),
    )
    for side, arrived_ref, plane_ref, touching, row, owner in sides:
        face_ref[side] = plane_ref[...]

        def add(data, force):
            corner = data[21:24, :].astype(i32)
            wy = window(data[9:15], corner[1:2], cells_y)
            wzh, wzl = halves(window(data[15:21], corner[2:3], cells_z))
            wx = jnp.where(corner[0:1] == touching, data[3 + row : 4 + row], 0.0)
            force = force * wx
            high, low = halves(jnp.concatenate([force[c : c + 1] * wy for c in range(3)], axis=0))
            face_ref[side] += dot3(high, low, wzh, wzl, NT).reshape(3, cells_y, cells_z)

        if quartered:
            capacity = slots // n_stream
            width = tile // n_stream
            for k in range(n_stream):
                marks_ref[side, k] = arrived_ref[k]
                marks_ref[side, k, 0:3] = given_ref[owner, :, k * capacity : (k + 1) * capacity]
            held = marks_ref[side]
            touches = (held[:, 21, :] == float(touching)) & (held[:, 3, :] != 0.0)
            lane = lax.broadcasted_iota(i32, touches.shape, 1)
            depth = lane + 1 if side else capacity - lane
            reach = jnp.max(jnp.where(touches, depth.astype(f32), 0.0)).astype(i32)
            per = capacity // width

            def step(index, _):
                data = quarter(marks_ref, side, index if side else per - 1 - index, width)
                add(data, data[0:3])

            lax.fori_loop(0, lax.div(reach + width - 1, width), step, None)
        else:
            for at, data in tiles_of(arrived_ref, tile, slots):
                add(data, given_ref[owner, :, at])
    y = lax.broadcasted_iota(i32, (cells_y, cells_z), 0)
    lower = jnp.where(wall == 0, 0.0, 1.0).astype(f32)
    upper = jnp.where(wall == n_wall - 1, 0.0, 1.0).astype(f32)
    scale = 1.0 / (1.0 + 6.0 * diffusion)
    for c in range(3):
        loads[c].wait()
        for x in range(cells_x):
            cell = rhs_ref[c, x]
            back = rhs_ref[c, x - 1] if x else face_ref[0, c]
            ahead = rhs_ref[c, x + 1] if x < cells_x - 1 else face_ref[1, c]
            below = jnp.where(y == 0, y0_ref[c, x : x + 1, :] * lower, pltpu.roll(cell, 1, 0))
            above = jnp.where(y == cells_y - 1, y1_ref[c, x : x + 1, :] * upper, pltpu.roll(cell, cells_y - 1, 0))
            side = pltpu.roll(cell, 1, 1) + pltpu.roll(cell, cells_z - 1, 1)
            near = (ahead + back) + (above + below) + side
            next_ref[c, x] = (cell + diffusion * near) * scale
        stores[c].start()
    if chunked:
        capacity = slots // n_stream
        mine = span(here, capacity)
        held = jnp.concatenate([given_ref[k, :, mine] for k in range(n_stream)], axis=1)
    else:
        held = held_ref[...]
    held = jnp.concatenate([held, jnp.zeros((5, slots), f32)], axis=0)
    moved = dot(thirds(held), one_hot(pos_ref[...], slots))
    moved = moved[0:8] + moved[8:16] + moved[16:24]
    force_ref[...] = moved[0:3]
    for store in stores:
        store.wait()


def per_device(velocity, target, weights, corners, dest):
    n_stream = lax.axis_size("gx")
    n_wall = lax.axis_size("gy")
    owned = target.shape[1]
    capacity = max(SLOT_MIN, 2 * owned // n_stream)
    slots = n_stream * capacity
    _, cells_x, cells_y, cells_z = velocity.shape
    block = cells_x * cells_y
    chunked = capacity % 128 == 0
    tile = 256 if slots % 256 == 0 else 128
    quartered = capacity == 128 and tile % n_stream == 0 and capacity % (tile // n_stream) == 0
    shape = jax.ShapeDtypeStruct
    sems = pltpu.SemaphoreType.DMA

    face_x = shape((3, cells_y, cells_z), f32)
    outgoing, position, x0, x1 = pl.pallas_call(
        functools.partial(pack_kernel, capacity, chunked),
        out_shape=(
            shape((n_stream, ROWS, capacity) if chunked else (ROWS, slots), f32),
            shape((1, owned), i32),
            face_x,
            face_x,
        ),
        in_specs=[VMEM] * 4 + [HBM],
        out_specs=(VMEM, VMEM, HBM, HBM),
        scratch_shapes=[pltpu.VMEM((ROWS, owned), f32), sems((2,))],
        name="pack",
    )(dest.reshape(1, owned), target, weights, corners, velocity)
    if chunked:
        arrived = lax.all_to_all(outgoing, "gx", split_axis=0, concat_axis=0, tiled=True)
    else:
        outgoing = outgoing.reshape(ROWS, n_stream, capacity)
        arrived = lax.all_to_all(outgoing, "gx", split_axis=1, concat_axis=1, tiled=True)
        arrived = arrived.reshape(ROWS, slots)

    high, low = pl.pallas_call(
        split_kernel,
        grid=(3,),
        out_shape=(shape((3, block, cells_z), bf16),) * 2,
        in_specs=[pl.BlockSpec((1, cells_x, cells_y, cells_z), lambda c: (c, 0, 0, 0))],
        out_specs=(pl.BlockSpec((1, block, cells_z), lambda c: (c, 0, 0)),) * 2,
        name="split",
    )(velocity)

    up_x = [(i, (i + 1) % n_stream) for i in range(n_stream)]
    down_x = [(j, i) for i, j in up_x]
    up_y = [(i, (i + 1) % n_wall) for i in range(n_wall)]
    down_y = [(j, i) for i, j in up_y]
    from_x0 = lax.ppermute(x1, "gx", up_x)
    from_x1 = lax.ppermute(x0, "gx", down_x)
    left = lax.ppermute(arrived, "gx", up_x)
    right = lax.ppermute(arrived, "gx", down_x)

    pad = -(-cells_x // 16) * 16
    force, wzh, wzl, wy, fx, y0, y1 = pl.pallas_call(
        functools.partial(sample_kernel, tile),
        out_shape=(
            shape((n_stream, 3, slots), f32),
            shape((cells_z, slots), bf16),
            shape((cells_z, slots), bf16),
            shape((cells_y, slots), f32),
            shape((3, cells_x, slots), f32),
            shape((3, cells_x, cells_z), f32),
            shape((3, cells_x, cells_z), f32),
        ),
        in_specs=[VMEM, HBM, HBM, HBM],
        out_specs=(VMEM, HBM, HBM, VMEM, VMEM, VMEM, VMEM),
        scratch_shapes=[
            pltpu.VMEM((3, block, cells_z), bf16),
            pltpu.VMEM((3, block, cells_z), bf16),
            pltpu.VMEM((3, cells_x, 8, cells_z), f32),
            pltpu.VMEM((3, cells_x, 8, cells_z), f32),
            pltpu.VMEM((cells_z, slots), bf16),
            pltpu.VMEM((cells_z, slots), bf16),
            pltpu.VMEM((6 * pad, slots), bf16),
            pltpu.VMEM((6 * pad, slots), bf16),
            sems((2, 3)),
            sems((2,)),
            sems((2,)),
        ],
        compiler_params=pltpu.CompilerParams(vmem_limit_bytes=63_280_000),
        name="sample",
    )(arrived, high, low, velocity)

    from_y0 = lax.ppermute(y1, "gy", up_y)
    from_y1 = lax.ppermute(y0, "gy", down_y)
    given = lax.all_to_all(force, "gx", split_axis=0, concat_axis=0, tiled=True)
    if chunked:
        held = position
    else:
        held = lax.dynamic_slice_in_dim(given, lax.axis_index("gx") * capacity, capacity, axis=2)
        held = held.transpose(1, 0, 2).reshape(3, slots)

    rhs = pl.pallas_call(
        spread_kernel,
        out_shape=shape(velocity.shape, f32),
        in_specs=[HBM, VMEM, VMEM, VMEM, VMEM],
        out_specs=HBM,
        scratch_shapes=[
            pltpu.VMEM((block, slots), bf16),
            pltpu.VMEM((block, slots), bf16),
            pltpu.VMEM(velocity.shape, f32),
            sems((3,)),
            sems((3,)),
        ],
        cost_estimate=pl.CostEstimate(flops=18 * block * slots * cells_z, bytes_accessed=24 * block * cells_z, transcendentals=0),
        name="spread",
    )(velocity, wzh, wzl, wy, fx)

    return pl.pallas_call(
        functools.partial(finish_kernel, tile, n_stream, n_wall, chunked, quartered),
        out_shape=(shape(velocity.shape, f32), shape((3, owned), f32)),
        in_specs=[HBM] + [VMEM] * 9,
        out_specs=(HBM, VMEM),
        scratch_shapes=[
            pltpu.VMEM(velocity.shape, f32),
            pltpu.VMEM(velocity.shape, f32),
            pltpu.VMEM((2, 3, cells_y, cells_z), f32),
            pltpu.VMEM((2, n_stream, ROWS, 128), f32),
            sems((3,)),
            sems((3,)),
        ],
        compiler_params=pltpu.CompilerParams(vmem_limit_bytes=62_400_000),
        name="finish",
    )(rhs, from_x0, from_x1, from_y0, from_y1, left, right, given, held, position)


def solution(mesh):
    in_specs = (
        P(None, "gx", "gy", None),
        P(None, ("gx", "gy")),
        P(None, None, ("gx", "gy")),
        P(None, ("gx", "gy")),
        P(("gx", "gy"), None),
    )
    out_specs = (P(None, "gx", "gy", None), P(None, ("gx", "gy")))
    return jax.shard_map(
        per_device, mesh=mesh, in_specs=in_specs, out_specs=out_specs, check_vma=False
    )
```

```python
import functools

import jax
import jax.numpy as jnp
from jax import lax
from jax.experimental import pallas as pl
from jax.experimental.pallas import tpu as pltpu
from jax.sharding import PartitionSpec as P


SLOT_MIN = 12
SPAN = 6
ROWS = 24

diffusion = 0.4


f32 = jnp.float32
bf16 = jnp.bfloat16
i32 = jnp.int32
VMEM = pl.BlockSpec(memory_space=pltpu.VMEM)
HBM = pl.BlockSpec(memory_space=pltpu.HBM)
NN = (((1,), (0,)), ((), ()))
NT = (((1,), (1,)), ((), ()))


def dot(a, b, dims=NN):
    return lax.dot_general(a, b, dims, preferred_element_type=f32)


def halves(x):
    high = x.astype(bf16)
    return high, (x - high.astype(f32)).astype(bf16)


def dot3(ah, al, bh, bl, dims=NN):
    return dot(ah, bh, dims) + dot(ah, bl, dims) + dot(al, bh, dims)


def thirds(x):
    high = x.astype(bf16).astype(f32)
    rest = x - high
    mid = rest.astype(bf16).astype(f32)
    return jnp.concatenate([high, mid, rest - mid], axis=0).astype(bf16)


def one_hot(position, slots):
    rows = lax.broadcasted_iota(i32, (slots, position.shape[1]), 0)
    return jnp.where(rows == position, 1.0, 0.0).astype(bf16)


def span(index, size):
    return pl.ds(pl.multiple_of(index * size, size), size)


def pack_kernel(
    capacity, chunked, dest_ref, target_ref, weights_ref, corners_ref, velocity_hbm,
    out_ref, pos_ref, x0_ref, x1_ref, rows_ref, sem,
):
    owned = target_ref.shape[1]
    cells_x = velocity_hbm.shape[1]
    faces = [
        pltpu.make_async_copy(velocity_hbm.at[:, 0], x0_ref, sem.at[0]),
        pltpu.make_async_copy(velocity_hbm.at[:, cells_x - 1], x1_ref, sem.at[1]),
    ]
    for face in faces:
        face.start()
    dest = dest_ref[...]
    corner = corners_ref[0:1, :]
    lane = lax.broadcasted_iota(i32, (1, owned), 1)
    last = corner == cells_x - SPAN
    group = jnp.where(last, 2, jnp.where(corner == 0, 0, 1))
    first = (dest * 4 + jnp.where(last, 2, 0)) * owned
    key = (dest * 4 + group) * owned + lane
    column = jnp.transpose(jnp.broadcast_to(key, (8, owned)))[:, 0:1]
    ahead = jnp.where((column < key) & (column >= first), 1.0, 0.0)
    rank = jnp.sum(ahead, axis=0, keepdims=True).astype(i32)
    position = dest * capacity + jnp.where(last, capacity - 1 - rank, rank)
    pos_ref[...] = position
    rows_ref[0:3, :] = target_ref[...]
    for dim in range(3):
        rows_ref[3 + 6 * dim : 9 + 6 * dim, :] = weights_ref[dim]
    rows_ref[21:24, :] = corners_ref[...].astype(f32)
    slots = out_ref.size // ROWS
    moved = dot(thirds(rows_ref[...]), one_hot(position, slots), NT)
    moved = moved[0:ROWS] + moved[ROWS : 2 * ROWS] + moved[2 * ROWS :]
    if chunked:
        for chunk in range(slots // capacity):
            out_ref[chunk] = moved[:, chunk * capacity : (chunk + 1) * capacity]
    else:
        out_ref[...] = moved
    for face in faces:
        face.wait()


def window(weights, corner, length):
    offset = lax.broadcasted_iota(i32, (length, weights.shape[1]), 0) - corner
    out = jnp.zeros(offset.shape, f32)
    for k in range(SPAN):
        out = jnp.where(offset == k, weights[k : k + 1, :], out)
    return out


def tiles_of(arrived_ref, tile, slots):
    for t in range(slots // tile):
        at = slice(t * tile, (t + 1) * tile)
        if len(arrived_ref.shape) == 3:
            per = tile // arrived_ref.shape[2]
            yield at, jnp.concatenate([arrived_ref[t * per + k] for k in range(per)], axis=1)
        else:
            yield at, arrived_ref[:, at]


def sample_kernel(
    tile, arrived_ref, velocity_hbm,
    force_ref, wzh_hbm, wzl_hbm, wy_ref, fx_ref, y0_ref, y1_ref,
    cell_ref, high_ref, low_ref, wzh_ref, wzl_ref, boxh_ref, boxl_ref, in_sem, out_sem,
):
    cells_x, cells_z = y0_ref.shape[1:]
    cells_y, slots = wy_ref.shape
    loads = [pltpu.make_async_copy(velocity_hbm.at[c], cell_ref.at[c], in_sem.at[c]) for c in range(3)]
    for load in loads:
        load.start()
    kept = []
    for at, data in tiles_of(arrived_ref, tile, slots):
        corner = data[21:24, :].astype(i32)
        wy_ref[:, at] = window(data[9:15], corner[1:2], cells_y)
        high, low = halves(window(data[15:21], corner[2:3], cells_z))
        wzh_ref[:, at] = high
        wzl_ref[:, at] = low
        kept.append((at, data[0:3], window(data[3:9], corner[0:1], cells_x)))
    stores = [
        pltpu.make_async_copy(wzh_ref, wzh_hbm, out_sem.at[0]),
        pltpu.make_async_copy(wzl_ref, wzl_hbm, out_sem.at[1]),
    ]
    for store in stores:
        store.start()
    for c in range(3):
        loads[c].wait()
        high, low = halves(cell_ref[c].reshape(cells_x * cells_y, cells_z))
        high_ref[c] = high
        low_ref[c] = low
        for at, target, wx in kept:
            along = dot3(high_ref[c], low_ref[c], wzh_ref[:, at], wzl_ref[:, at])
            along = along.reshape(cells_x, cells_y, tile) * wy_ref[:, at][None]
            sampled = jnp.sum(jnp.sum(along, axis=1) * wx, axis=0, keepdims=True)
            force = target[c : c + 1] - sampled
            fx_ref[c, :, at] = force * wx
            for k in range(force_ref.shape[0]):
                force_ref[k, c : c + 1, at] = force
    pad = boxh_ref.shape[0] // 6
    base = 0
    for y in (0, cells_y - 1):
        for c in range(3):
            rows = fx_ref[c] * wy_ref[y : y + 1, :]
            rows = jnp.concatenate([rows, jnp.zeros((pad - cells_x, slots), f32)], axis=0)
            high, low = halves(rows)
            boxh_ref[base : base + pad] = high
            boxl_ref[base : base + pad] = low
            base += pad
    spread = dot3(boxh_ref[...], boxl_ref[...], wzh_ref[...], wzl_ref[...], NT)
    base = 0
    for y, ref in ((0, y0_ref), (cells_y - 1, y1_ref)):
        for c in range(3):
            ref[c] = cell_ref[c, :, y, :] + spread[base : base + cells_x]
            base += pad
    for store in stores:
        store.wait()


def spread_kernel(
    velocity_hbm, wzh_ref, wzl_ref, wy_ref, fx_ref, rhs_hbm, boxh_ref, boxl_ref, cell_ref, in_sem, out_sem,
):
    _, cells_x, cells_y, cells_z = velocity_hbm.shape
    loads = [pltpu.make_async_copy(velocity_hbm.at[c], cell_ref.at[c], in_sem.at[c]) for c in range(3)]
    stores = [pltpu.make_async_copy(cell_ref.at[c], rhs_hbm.at[c], out_sem.at[c]) for c in range(3)]
    for load in loads:
        load.start()
    wy = wy_ref[...]
    for c in range(3):
        for x in range(cells_x):
            high, low = halves(fx_ref[c, x : x + 1, :] * wy)
            boxh_ref[x * cells_y : (x + 1) * cells_y] = high
            boxl_ref[x * cells_y : (x + 1) * cells_y] = low
        spread = dot3(boxh_ref[...], boxl_ref[...], wzh_ref[...], wzl_ref[...], NT)
        loads[c].wait()
        cell_ref[c] = cell_ref[c] + spread.reshape(cells_x, cells_y, cells_z)
        stores[c].start()
    for store in stores:
        store.wait()


def quarter(marks_ref, side, index, width):
    lane = lax.broadcasted_iota(i32, marks_ref.shape[2:], 1)
    capacity = marks_ref.shape[3]
    per = capacity // width
    out = []
    for base in range(0, marks_ref.shape[1], per):
        piece = jnp.zeros(marks_ref.shape[2:], f32)
        for k in range(per):
            moved = pltpu.roll(marks_ref[side, base + k], lax.rem(capacity + (k - index) * width, capacity), 1)
            piece = jnp.where((lane >= k * width) & (lane < (k + 1) * width), moved, piece)
        out.append(piece)
    return jnp.concatenate(out, axis=1)


def finish_kernel(
    tile, n_stream, n_wall, chunked, quartered,
    rhs_hbm, x0_ref, x1_ref, y0_ref, y1_ref, left_ref, right_ref, given_ref, held_ref, pos_ref,
    next_hbm, force_ref, rhs_ref, next_ref, face_ref, marks_ref, in_sem, out_sem,
):
    _, cells_x, cells_y, cells_z = rhs_hbm.shape
    slots = given_ref.shape[2]
    loads = [pltpu.make_async_copy(rhs_hbm.at[c], rhs_ref.at[c], in_sem.at[c]) for c in range(3)]
    stores = [pltpu.make_async_copy(next_ref.at[c], next_hbm.at[c], out_sem.at[c]) for c in range(3)]
    for load in loads:
        load.start()
    here = lax.axis_index("gx")
    wall = lax.axis_index("gy")
    sides = (
        (0, left_ref, x0_ref, cells_x - SPAN, SPAN - 1, lax.rem(here + n_stream - 1, n_stream)),
        (1, right_ref, x1_ref, 0, 0, lax.rem(here + 1, n_stream)),
    )
    for side, arrived_ref, plane_ref, touching, row, owner in sides:
        face_ref[side] = plane_ref[...]

        def add(data, force):
            corner = data[21:24, :].astype(i32)
            wy = window(data[9:15], corner[1:2], cells_y)
            wzh, wzl = halves(window(data[15:21], corner[2:3], cells_z))
            wx = jnp.where(corner[0:1] == touching, data[3 + row : 4 + row], 0.0)
            force = force * wx
            high, low = halves(jnp.concatenate([force[c : c + 1] * wy for c in range(3)], axis=0))
            face_ref[side] += dot3(high, low, wzh, wzl, NT).reshape(3, cells_y, cells_z)

        if quartered:
            capacity = slots // n_stream
            width = tile // n_stream
            for k in range(n_stream):
                marks_ref[side, k] = arrived_ref[k]
                marks_ref[side, k, 0:3] = given_ref[owner, :, k * capacity : (k + 1) * capacity]
            held = marks_ref[side]
            touches = (held[:, 21, :] == float(touching)) & (held[:, 3, :] != 0.0)
            lane = lax.broadcasted_iota(i32, touches.shape, 1)
            depth = lane + 1 if side else capacity - lane
            reach = jnp.max(jnp.where(touches, depth.astype(f32), 0.0)).astype(i32)
            per = capacity // width

            def step(index, _):
                data = quarter(marks_ref, side, index if side else per - 1 - index, width)
                add(data, data[0:3])

            lax.fori_loop(0, lax.div(reach + width - 1, width), step, None)
        else:
            for at, data in tiles_of(arrived_ref, tile, slots):
                add(data, given_ref[owner, :, at])
    y = lax.broadcasted_iota(i32, (cells_y, cells_z), 0)
    lower = jnp.where(wall == 0, 0.0, 1.0).astype(f32)
    upper = jnp.where(wall == n_wall - 1, 0.0, 1.0).astype(f32)
    scale = 1.0 / (1.0 + 6.0 * diffusion)
    for c in range(3):
        loads[c].wait()
        for x in range(cells_x):
            cell = rhs_ref[c, x]
            back = rhs_ref[c, x - 1] if x else face_ref[0, c]
            ahead = rhs_ref[c, x + 1] if x < cells_x - 1 else face_ref[1, c]
            below = jnp.where(y == 0, y0_ref[c, x : x + 1, :] * lower, pltpu.roll(cell, 1, 0))
            above = jnp.where(y == cells_y - 1, y1_ref[c, x : x + 1, :] * upper, pltpu.roll(cell, cells_y - 1, 0))
            side = pltpu.roll(cell, 1, 1) + pltpu.roll(cell, cells_z - 1, 1)
            near = (ahead + back) + (above + below) + side
            next_ref[c, x] = (cell + diffusion * near) * scale
        stores[c].start()
    if chunked:
        capacity = slots // n_stream
        mine = span(here, capacity)
        held = jnp.concatenate([given_ref[k, :, mine] for k in range(n_stream)], axis=1)
    else:
        held = held_ref[...]
    held = jnp.concatenate([held, jnp.zeros((5, slots), f32)], axis=0)
    moved = dot(thirds(held), one_hot(pos_ref[...], slots))
    moved = moved[0:8] + moved[8:16] + moved[16:24]
    force_ref[...] = moved[0:3]
    for store in stores:
        store.wait()


def per_device(velocity, target, weights, corners, dest):
    n_stream = lax.axis_size("gx")
    n_wall = lax.axis_size("gy")
    owned = target.shape[1]
    capacity = max(SLOT_MIN, 2 * owned // n_stream)
    slots = n_stream * capacity
    _, cells_x, cells_y, cells_z = velocity.shape
    block = cells_x * cells_y
    chunked = capacity % 128 == 0
    tile = 256 if slots % 256 == 0 else 128
    quartered = capacity == 128 and tile % n_stream == 0 and capacity % (tile // n_stream) == 0
    shape = jax.ShapeDtypeStruct
    sems = pltpu.SemaphoreType.DMA

    face_x = shape((3, cells_y, cells_z), f32)
    outgoing, position, x0, x1 = pl.pallas_call(
        functools.partial(pack_kernel, capacity, chunked),
        out_shape=(
            shape((n_stream, ROWS, capacity) if chunked else (ROWS, slots), f32),
            shape((1, owned), i32),
            face_x,
            face_x,
        ),
        in_specs=[VMEM] * 4 + [HBM],
        out_specs=(VMEM,) * 4,
        scratch_shapes=[pltpu.VMEM((ROWS, owned), f32), sems((2,))],
        name="pack",
    )(dest.reshape(1, owned), target, weights, corners, velocity)
    if chunked:
        arrived = lax.all_to_all(outgoing, "gx", split_axis=0, concat_axis=0, tiled=True)
    else:
        outgoing = outgoing.reshape(ROWS, n_stream, capacity)
        arrived = lax.all_to_all(outgoing, "gx", split_axis=1, concat_axis=1, tiled=True)
        arrived = arrived.reshape(ROWS, slots)

    up_x = [(i, (i + 1) % n_stream) for i in range(n_stream)]
    down_x = [(j, i) for i, j in up_x]
    up_y = [(i, (i + 1) % n_wall) for i in range(n_wall)]
    down_y = [(j, i) for i, j in up_y]
    from_x0 = lax.ppermute(x1, "gx", up_x)
    from_x1 = lax.ppermute(x0, "gx", down_x)
    left = lax.ppermute(arrived, "gx", up_x)
    right = lax.ppermute(arrived, "gx", down_x)

    pad = -(-cells_x // 16) * 16
    force, wzh, wzl, wy, fx, y0, y1 = pl.pallas_call(
        functools.partial(sample_kernel, tile),
        out_shape=(
            shape((n_stream, 3, slots), f32),
            shape((cells_z, slots), bf16),
            shape((cells_z, slots), bf16),
            shape((cells_y, slots), f32),
            shape((3, cells_x, slots), f32),
            shape((3, cells_x, cells_z), f32),
            shape((3, cells_x, cells_z), f32),
        ),
        in_specs=[VMEM, HBM],
        out_specs=(VMEM, HBM, HBM, VMEM, VMEM, VMEM, VMEM),
        scratch_shapes=[
            pltpu.VMEM(velocity.shape, f32),
            pltpu.VMEM((3, block, cells_z), bf16),
            pltpu.VMEM((3, block, cells_z), bf16),
            pltpu.VMEM((cells_z, slots), bf16),
            pltpu.VMEM((cells_z, slots), bf16),
            pltpu.VMEM((6 * pad, slots), bf16),
            pltpu.VMEM((6 * pad, slots), bf16),
            sems((3,)),
            sems((2,)),
        ],
        compiler_params=pltpu.CompilerParams(vmem_limit_bytes=63_280_000),
        name="sample",
    )(arrived, velocity)

    from_y0 = lax.ppermute(y1, "gy", up_y)
    from_y1 = lax.ppermute(y0, "gy", down_y)
    given = lax.all_to_all(force, "gx", split_axis=0, concat_axis=0, tiled=True)
    if chunked:
        held = position
    else:
        held = lax.dynamic_slice_in_dim(given, lax.axis_index("gx") * capacity, capacity, axis=2)
        held = held.transpose(1, 0, 2).reshape(3, slots)

    rhs = pl.pallas_call(
        spread_kernel,
        out_shape=shape(velocity.shape, f32),
        in_specs=[HBM, VMEM, VMEM, VMEM, VMEM],
        out_specs=HBM,
        scratch_shapes=[
            pltpu.VMEM((block, slots), bf16),
            pltpu.VMEM((block, slots), bf16),
            pltpu.VMEM(velocity.shape, f32),
            sems((3,)),
            sems((3,)),
        ],
        cost_estimate=pl.CostEstimate(flops=18 * block * slots * cells_z, bytes_accessed=24 * block * cells_z, transcendentals=0),
        name="spread",
    )(velocity, wzh, wzl, wy, fx)

    return pl.pallas_call(
        functools.partial(finish_kernel, tile, n_stream, n_wall, chunked, quartered),
        out_shape=(shape(velocity.shape, f32), shape((3, owned), f32)),
        in_specs=[HBM] + [VMEM] * 9,
        out_specs=(HBM, VMEM),
        scratch_shapes=[
            pltpu.VMEM(velocity.shape, f32),
            pltpu.VMEM(velocity.shape, f32),
            pltpu.VMEM((2, 3, cells_y, cells_z), f32),
            pltpu.VMEM((2, n_stream, ROWS, 128), f32),
            sems((3,)),
            sems((3,)),
        ],
        compiler_params=pltpu.CompilerParams(vmem_limit_bytes=62_400_000),
        name="finish",
    )(rhs, from_x0, from_x1, from_y0, from_y1, left, right, given, held, position)


def solution(mesh):
    in_specs = (
        P(None, "gx", "gy", None),
        P(None, ("gx", "gy")),
        P(None, None, ("gx", "gy")),
        P(None, ("gx", "gy")),
        P(("gx", "gy"), None),
    )
    out_specs = (P(None, "gx", "gy", None), P(None, ("gx", "gy")))
    return jax.shard_map(
        per_device, mesh=mesh, in_specs=in_specs, out_specs=out_specs, check_vma=False
    )
```

```python
import functools

import jax
import jax.numpy as jnp
from jax import lax
from jax.experimental import pallas as pl
from jax.experimental.pallas import tpu as pltpu
from jax.sharding import PartitionSpec as P


SLOT_MIN = 12
SPAN = 6
ROWS = 24

diffusion = 0.4


f32 = jnp.float32
bf16 = jnp.bfloat16
i32 = jnp.int32
VMEM = pl.BlockSpec(memory_space=pltpu.VMEM)
SMEM = pl.BlockSpec(memory_space=pltpu.SMEM)
HBM = pl.BlockSpec(memory_space=pltpu.HBM)
NN = (((1,), (0,)), ((), ()))
NT = (((1,), (1,)), ((), ()))


def dot(a, b, dims=NN):
    return lax.dot_general(a, b, dims, preferred_element_type=f32)


def halves(x):
    high = x.astype(bf16)
    return high, (x - high.astype(f32)).astype(bf16)


def dot3(ah, al, bh, bl, dims=NN):
    return dot(ah, bh, dims) + dot(ah, bl, dims) + dot(al, bh, dims)


def thirds(x):
    high = x.astype(bf16).astype(f32)
    rest = x - high
    mid = rest.astype(bf16).astype(f32)
    return jnp.concatenate([high, mid, rest - mid], axis=0).astype(bf16)


def one_hot(position, slots):
    rows = lax.broadcasted_iota(i32, (slots, position.shape[1]), 0)
    return jnp.where(rows == position, 1.0, 0.0).astype(bf16)


def span(index, size):
    return pl.ds(pl.multiple_of(index * size, size), size)


def pack_kernel(
    capacity, chunked, dest_ref, target_ref, weights_ref, corners_ref, velocity_hbm,
    out_ref, pos_ref, x0_ref, x1_ref, rows_ref, sem,
):
    owned = target_ref.shape[1]
    cells_x = velocity_hbm.shape[1]
    faces = [
        pltpu.make_async_copy(velocity_hbm.at[:, 0], x0_ref, sem.at[0]),
        pltpu.make_async_copy(velocity_hbm.at[:, cells_x - 1], x1_ref, sem.at[1]),
    ]
    for face in faces:
        face.start()
    dest = dest_ref[...]
    corner = corners_ref[0:1, :]
    lane = lax.broadcasted_iota(i32, (1, owned), 1)
    top = cells_x - SPAN
    last = corner > top // 2
    first = (dest * 2 + jnp.where(last, 1, 0)) * (cells_x * owned)
    key = first + jnp.where(last, top - corner, corner) * owned + lane
    column = jnp.transpose(jnp.broadcast_to(key, (8, owned)))[:, 0:1]
    ahead = jnp.where((column < key) & (column >= first), 1.0, 0.0)
    rank = jnp.sum(ahead, axis=0, keepdims=True).astype(i32)
    position = dest * capacity + jnp.where(last, capacity - 1 - rank, rank)
    pos_ref[...] = position
    rows_ref[0:3, :] = target_ref[...]
    for dim in range(3):
        rows_ref[3 + 6 * dim : 9 + 6 * dim, :] = weights_ref[dim]
    rows_ref[21:24, :] = corners_ref[...].astype(f32)
    slots = out_ref.size // ROWS
    moved = dot(thirds(rows_ref[...]), one_hot(position, slots), NT)
    moved = moved[0:ROWS] + moved[ROWS : 2 * ROWS] + moved[2 * ROWS :]
    if chunked:
        for chunk in range(slots // capacity):
            out_ref[chunk] = moved[:, chunk * capacity : (chunk + 1) * capacity]
    else:
        out_ref[...] = moved
    for face in faces:
        face.wait()


def window(weights, corner, length):
    offset = lax.broadcasted_iota(i32, (length, weights.shape[1]), 0) - corner
    out = jnp.zeros(offset.shape, f32)
    for k in range(SPAN):
        out = jnp.where(offset == k, weights[k : k + 1, :], out)
    return out


def tiles_of(arrived_ref, tile, slots):
    for t in range(slots // tile):
        at = slice(t * tile, (t + 1) * tile)
        if len(arrived_ref.shape) == 3:
            per = tile // arrived_ref.shape[2]
            yield at, jnp.concatenate([arrived_ref[t * per + k] for k in range(per)], axis=1)
        else:
            yield at, arrived_ref[:, at]


def quarter(chunk, chunks, capacity, index, width):
    lane = lax.broadcasted_iota(i32, (ROWS, capacity), 1)
    per = capacity // width
    out = []
    for base in range(0, chunks, per):
        piece = jnp.zeros((ROWS, capacity), f32)
        for k in range(per):
            moved = pltpu.roll(chunk(base + k), lax.rem(capacity + (k - index) * width, capacity), 1)
            piece = jnp.where((lane >= k * width) & (lane < (k + 1) * width), moved, piece)
        out.append(piece)
    return jnp.concatenate(out, axis=1)


def sample_kernel(
    tile, n_stream, quartered, band, arrived_ref, velocity_hbm,
    force_ref, wzh_hbm, wzl_hbm, wy_ref, fx_ref, y0_ref, y1_ref, start_ref,
    cell_ref, high_ref, low_ref, wzh_ref, wzl_ref, wx_ref, rel_ref, goal_ref, face_ref, in_sem, out_sem,
):
    cells_x, cells_z = y0_ref.shape[1:]
    cells_y, slots = wy_ref.shape
    pad = wx_ref.shape[0]
    count = slots // tile
    capacity = slots // n_stream
    width = tile // n_stream
    loads = [pltpu.make_async_copy(velocity_hbm.at[c], cell_ref.at[c], in_sem.at[c]) for c in range(3)]
    for load in loads:
        load.start()

    def tile_data(t):
        if quartered:
            return quarter(lambda k: arrived_ref[k], n_stream, capacity, t, width)
        if len(arrived_ref.shape) == 3:
            per = tile // capacity
            return jnp.concatenate([arrived_ref[t * per + k] for k in range(per)], axis=1)
        return arrived_ref[:, t * tile : (t + 1) * tile]

    kept = []
    fits = None
    for t in range(count):
        at = slice(t * tile, (t + 1) * tile)
        data = tile_data(t)
        corner = data[21:24, :].astype(i32)
        if quartered:
            used = data[3:4] != 0.0
            low = jnp.min(jnp.where(used, data[21:22], float(cells_x))).astype(i32)
            high = jnp.max(jnp.where(used, data[21:22], -1.0)).astype(i32)
            start = jnp.minimum(low, cells_x - band)
            inside = high + SPAN <= start + band
            fits = inside if fits is None else fits & inside
        else:
            start = 0
        kept.append((at, data, corner, start))
        wy_ref[:, at] = window(data[9:15], corner[1:2], cells_y)
        high, low = halves(window(data[15:21], corner[2:3], cells_z))
        wzh_ref[:, at] = high
        wzl_ref[:, at] = low
        for c in range(3):
            goal_ref[c, 0:1, at] = data[c : c + 1]
    stores = [
        pltpu.make_async_copy(wzh_ref, wzh_hbm, out_sem.at[0]),
        pltpu.make_async_copy(wzl_ref, wzl_hbm, out_sem.at[1]),
    ]
    for store in stores:
        store.start()
    if not quartered:
        fits = jnp.bool_(False)
    for t, (at, data, corner, start) in enumerate(kept):
        start = jnp.where(fits, start, 0)
        start_ref[t] = start
        wx_ref[:, at] = window(data[3:9], corner[0:1], pad)
        rel_ref[:, at] = window(data[3:9], corner[0:1] - start, pad)
    start_ref[count] = jnp.where(fits, 1, 0)
    for c in range(3):
        loads[c].wait()
        high, low = halves(cell_ref[c].reshape(cells_x * cells_y, cells_z))
        high_ref[c] = high
        low_ref[c] = low

    def sample(planes):
        def step(t, _):
            at = span(t, tile)
            rows = pl.ds(pl.multiple_of(start_ref[t] * cells_y, cells_y), planes * cells_y)
            wx = rel_ref[:, at]
            wy = wy_ref[:, at]
            for c in range(3):
                along = dot3(high_ref[c, rows, :], low_ref[c, rows, :], wzh_ref[:, at], wzl_ref[:, at])
                along = along.reshape(planes, cells_y, tile) * wy[None]
                sampled = jnp.sum(jnp.sum(along, axis=1) * wx[0:planes], axis=0, keepdims=True)
                force = goal_ref[c, 0:1, at] - sampled
                fx_ref[c, :, at] = force * wx
                goal_ref[c, 0:1, at] = force

        lax.fori_loop(0, count, step, None)

    if quartered:
        pl.when(fits)(lambda: sample(band))
        pl.when(jnp.logical_not(fits))(lambda: sample(cells_x))
    else:
        sample(cells_x)
    forces = [goal_ref[c, 0:1, :] for c in range(3)]
    if quartered:
        lane = lax.broadcasted_iota(i32, (8, capacity), 1)
        mixed = jnp.concatenate(forces + [jnp.zeros((5, slots), f32)], axis=0)
        per = capacity // width
        own = []
        for k in range(n_stream):
            piece = jnp.zeros((8, capacity), f32)
            for t in range(count):
                base = t * tile + k // per * capacity
                moved = pltpu.roll(mixed[:, base : base + capacity], (t - k % per) * width % capacity, 1)
                piece = jnp.where((lane >= t * width) & (lane < (t + 1) * width), moved, piece)
            own.append(piece)
        natural = jnp.concatenate(own, axis=1)[0:3]
    else:
        natural = jnp.concatenate(forces, axis=0)
    for k in range(force_ref.shape[0]):
        force_ref[k] = natural
    face_ref[...] = jnp.zeros_like(face_ref)

    def edges(t, _):
        at = span(t, tile)
        wx = wx_ref[:, at]
        wy = wy_ref[:, at]
        rows = [goal_ref[c, 0:1, at] * wx * wy[y : y + 1] for y in (0, cells_y - 1) for c in range(3)]
        high, low = halves(jnp.concatenate(rows, axis=0))
        face_ref[...] += dot3(high, low, wzh_ref[:, at], wzl_ref[:, at], NT)

    lax.fori_loop(0, count, edges, None)
    base = 0
    for y, ref in ((0, y0_ref), (cells_y - 1, y1_ref)):
        for c in range(3):
            ref[c] = cell_ref[c, :, y, :] + face_ref[base : base + cells_x]
            base += pad
    for store in stores:
        store.wait()


def spread_kernel(
    tile, quartered, band, velocity_hbm, wzh_ref, wzl_ref, wy_ref, fx_ref, start_ref, rhs_hbm, cell_ref, in_sem, out_sem,
):
    _, cells_x, cells_y, cells_z = velocity_hbm.shape
    count = wy_ref.shape[1] // tile
    loads = [pltpu.make_async_copy(velocity_hbm.at[c], cell_ref.at[c], in_sem.at[c]) for c in range(3)]
    stores = [pltpu.make_async_copy(cell_ref.at[c], rhs_hbm.at[c], out_sem.at[c]) for c in range(3)]
    for load in loads:
        load.start()
    for load in loads:
        load.wait()

    def spread(planes):
        def step(t, _):
            at = span(t, tile)
            rows = pl.ds(start_ref[t], planes)
            wy = wy_ref[:, at]
            for c in range(3):
                boxes = jnp.concatenate([fx_ref[c, x : x + 1, at] * wy for x in range(planes)], axis=0)
                high, low = halves(boxes)
                added = dot3(high, low, wzh_ref[:, at], wzl_ref[:, at], NT)
                cell_ref[c, rows] += added.reshape(planes, cells_y, cells_z)

        lax.fori_loop(0, count, step, None)

    if quartered:
        fits = start_ref[count] == 1
        pl.when(fits)(lambda: spread(band))
        pl.when(jnp.logical_not(fits))(lambda: spread(cells_x))
    else:
        spread(cells_x)
    for store in stores:
        store.start()
    for store in stores:
        store.wait()


def finish_kernel(
    tile, n_stream, n_wall, chunked, quartered,
    rhs_hbm, x0_ref, x1_ref, y0_ref, y1_ref, left_ref, right_ref, given_ref, held_ref, pos_ref,
    next_hbm, force_ref, rhs_ref, next_ref, face_ref, marks_ref, in_sem, out_sem,
):
    _, cells_x, cells_y, cells_z = rhs_hbm.shape
    slots = given_ref.shape[2]
    loads = [pltpu.make_async_copy(rhs_hbm.at[c], rhs_ref.at[c], in_sem.at[c]) for c in range(3)]
    stores = [pltpu.make_async_copy(next_ref.at[c], next_hbm.at[c], out_sem.at[c]) for c in range(3)]
    for load in loads:
        load.start()
    here = lax.axis_index("gx")
    wall = lax.axis_index("gy")
    sides = (
        (0, left_ref, x0_ref, cells_x - SPAN, SPAN - 1, lax.rem(here + n_stream - 1, n_stream)),
        (1, right_ref, x1_ref, 0, 0, lax.rem(here + 1, n_stream)),
    )
    for side, arrived_ref, plane_ref, touching, row, owner in sides:
        face_ref[side] = plane_ref[...]

        def add(data, force):
            corner = data[21:24, :].astype(i32)
            wy = window(data[9:15], corner[1:2], cells_y)
            wzh, wzl = halves(window(data[15:21], corner[2:3], cells_z))
            wx = jnp.where(corner[0:1] == touching, data[3 + row : 4 + row], 0.0)
            force = force * wx
            high, low = halves(jnp.concatenate([force[c : c + 1] * wy for c in range(3)], axis=0))
            face_ref[side] += dot3(high, low, wzh, wzl, NT).reshape(3, cells_y, cells_z)

        if quartered:
            capacity = slots // n_stream
            width = tile // n_stream
            for k in range(n_stream):
                marks_ref[side, k] = arrived_ref[k]
                marks_ref[side, k, 0:3] = given_ref[owner, :, k * capacity : (k + 1) * capacity]
            held = marks_ref[side]
            touches = (held[:, 21, :] == float(touching)) & (held[:, 3, :] != 0.0)
            lane = lax.broadcasted_iota(i32, touches.shape, 1)
            depth = lane + 1 if side else capacity - lane
            reach = jnp.max(jnp.where(touches, depth.astype(f32), 0.0)).astype(i32)
            per = capacity // width

            def step(index, _):
                at = index if side else per - 1 - index
                data = quarter(lambda k: marks_ref[side, k], n_stream, capacity, at, width)
                add(data, data[0:3])

            lax.fori_loop(0, lax.div(reach + width - 1, width), step, None)
        else:
            for at, data in tiles_of(arrived_ref, tile, slots):
                add(data, given_ref[owner, :, at])
    y = lax.broadcasted_iota(i32, (cells_y, cells_z), 0)
    lower = jnp.where(wall == 0, 0.0, 1.0).astype(f32)
    upper = jnp.where(wall == n_wall - 1, 0.0, 1.0).astype(f32)
    scale = 1.0 / (1.0 + 6.0 * diffusion)
    for c in range(3):
        loads[c].wait()
        for x in range(cells_x):
            cell = rhs_ref[c, x]
            back = rhs_ref[c, x - 1] if x else face_ref[0, c]
            ahead = rhs_ref[c, x + 1] if x < cells_x - 1 else face_ref[1, c]
            below = jnp.where(y == 0, y0_ref[c, x : x + 1, :] * lower, pltpu.roll(cell, 1, 0))
            above = jnp.where(y == cells_y - 1, y1_ref[c, x : x + 1, :] * upper, pltpu.roll(cell, cells_y - 1, 0))
            side = pltpu.roll(cell, 1, 1) + pltpu.roll(cell, cells_z - 1, 1)
            near = (ahead + back) + (above + below) + side
            next_ref[c, x] = (cell + diffusion * near) * scale
        stores[c].start()
    if chunked:
        capacity = slots // n_stream
        mine = span(here, capacity)
        held = jnp.concatenate([given_ref[k, :, mine] for k in range(n_stream)], axis=1)
    else:
        held = held_ref[...]
    held = jnp.concatenate([held, jnp.zeros((5, slots), f32)], axis=0)
    moved = dot(thirds(held), one_hot(pos_ref[...], slots))
    moved = moved[0:8] + moved[8:16] + moved[16:24]
    force_ref[...] = moved[0:3]
    for store in stores:
        store.wait()


def per_device(velocity, target, weights, corners, dest):
    n_stream = lax.axis_size("gx")
    n_wall = lax.axis_size("gy")
    owned = target.shape[1]
    capacity = max(SLOT_MIN, 2 * owned // n_stream)
    slots = n_stream * capacity
    _, cells_x, cells_y, cells_z = velocity.shape
    block = cells_x * cells_y
    chunked = capacity % 128 == 0
    tile = 256 if slots % 256 == 0 else 128
    quartered = capacity == 128 and tile % n_stream == 0 and capacity % (tile // n_stream) == 0
    band = min(cells_x, SPAN + (cells_x - SPAN + 1) // 2)
    shape = jax.ShapeDtypeStruct
    sems = pltpu.SemaphoreType.DMA

    face_x = shape((3, cells_y, cells_z), f32)
    outgoing, position, x0, x1 = pl.pallas_call(
        functools.partial(pack_kernel, capacity, chunked),
        out_shape=(
            shape((n_stream, ROWS, capacity) if chunked else (ROWS, slots), f32),
            shape((1, owned), i32),
            face_x,
            face_x,
        ),
        in_specs=[VMEM] * 4 + [HBM],
        out_specs=(VMEM,) * 4,
        scratch_shapes=[pltpu.VMEM((ROWS, owned), f32), sems((2,))],
        name="pack",
    )(dest.reshape(1, owned), target, weights, corners, velocity)
    if chunked:
        arrived = lax.all_to_all(outgoing, "gx", split_axis=0, concat_axis=0, tiled=True)
    else:
        outgoing = outgoing.reshape(ROWS, n_stream, capacity)
        arrived = lax.all_to_all(outgoing, "gx", split_axis=1, concat_axis=1, tiled=True)
        arrived = arrived.reshape(ROWS, slots)

    up_x = [(i, (i + 1) % n_stream) for i in range(n_stream)]
    down_x = [(j, i) for i, j in up_x]
    up_y = [(i, (i + 1) % n_wall) for i in range(n_wall)]
    down_y = [(j, i) for i, j in up_y]
    from_x0 = lax.ppermute(x1, "gx", up_x)
    from_x1 = lax.ppermute(x0, "gx", down_x)
    left = lax.ppermute(arrived, "gx", up_x)
    right = lax.ppermute(arrived, "gx", down_x)

    pad = -(-cells_x // 16) * 16
    force, wzh, wzl, wy, fx, y0, y1, starts = pl.pallas_call(
        functools.partial(sample_kernel, tile, n_stream, quartered, band),
        out_shape=(
            shape((n_stream, 3, slots), f32),
            shape((cells_z, slots), bf16),
            shape((cells_z, slots), bf16),
            shape((cells_y, slots), f32),
            shape((3, pad, slots), f32),
            shape((3, cells_x, cells_z), f32),
            shape((3, cells_x, cells_z), f32),
            shape((slots // tile + 1,), i32),
        ),
        in_specs=[VMEM, HBM],
        out_specs=(VMEM, HBM, HBM, VMEM, VMEM, VMEM, VMEM, SMEM),
        scratch_shapes=[
            pltpu.VMEM(velocity.shape, f32),
            pltpu.VMEM((3, block, cells_z), bf16),
            pltpu.VMEM((3, block, cells_z), bf16),
            pltpu.VMEM((cells_z, slots), bf16),
            pltpu.VMEM((cells_z, slots), bf16),
            pltpu.VMEM((pad, slots), f32),
            pltpu.VMEM((pad, slots), f32),
            pltpu.VMEM((3, 8, slots), f32),
            pltpu.VMEM((6 * pad, cells_z), f32),
            sems((3,)),
            sems((2,)),
        ],
        compiler_params=pltpu.CompilerParams(vmem_limit_bytes=63_280_000),
        name="sample",
    )(arrived, velocity)

    from_y0 = lax.ppermute(y1, "gy", up_y)
    from_y1 = lax.ppermute(y0, "gy", down_y)
    given = lax.all_to_all(force, "gx", split_axis=0, concat_axis=0, tiled=True)
    if chunked:
        held = position
    else:
        held = lax.dynamic_slice_in_dim(given, lax.axis_index("gx") * capacity, capacity, axis=2)
        held = held.transpose(1, 0, 2).reshape(3, slots)

    rhs = pl.pallas_call(
        functools.partial(spread_kernel, tile, quartered, band),
        out_shape=shape(velocity.shape, f32),
        in_specs=[HBM, VMEM, VMEM, VMEM, VMEM, SMEM],
        out_specs=HBM,
        scratch_shapes=[
            pltpu.VMEM(velocity.shape, f32),
            sems((3,)),
            sems((3,)),
        ],
        cost_estimate=pl.CostEstimate(flops=18 * block * slots * cells_z, bytes_accessed=24 * block * cells_z, transcendentals=0),
        name="spread",
    )(velocity, wzh, wzl, wy, fx, starts)

    return pl.pallas_call(
        functools.partial(finish_kernel, tile, n_stream, n_wall, chunked, quartered),
        out_shape=(shape(velocity.shape, f32), shape((3, owned), f32)),
        in_specs=[HBM] + [VMEM] * 9,
        out_specs=(HBM, VMEM),
        scratch_shapes=[
            pltpu.VMEM(velocity.shape, f32),
            pltpu.VMEM(velocity.shape, f32),
            pltpu.VMEM((2, 3, cells_y, cells_z), f32),
            pltpu.VMEM((2, n_stream, ROWS, 128), f32),
            sems((3,)),
            sems((3,)),
        ],
        compiler_params=pltpu.CompilerParams(vmem_limit_bytes=62_400_000),
        name="finish",
    )(rhs, from_x0, from_x1, from_y0, from_y1, left, right, given, held, position)


def solution(mesh):
    in_specs = (
        P(None, "gx", "gy", None),
        P(None, ("gx", "gy")),
        P(None, None, ("gx", "gy")),
        P(None, ("gx", "gy")),
        P(("gx", "gy"), None),
    )
    out_specs = (P(None, "gx", "gy", None), P(None, ("gx", "gy")))
    return jax.shard_map(
        per_device, mesh=mesh, in_specs=in_specs, out_specs=out_specs, check_vma=False
    )
```

```python
import functools

import jax
import jax.numpy as jnp
from jax import lax
from jax.experimental import pallas as pl
from jax.experimental.pallas import tpu as pltpu
from jax.sharding import PartitionSpec as P


SLOT_MIN = 12
SPAN = 6
ROWS = 24

diffusion = 0.4


f32 = jnp.float32
bf16 = jnp.bfloat16
i32 = jnp.int32
VMEM = pl.BlockSpec(memory_space=pltpu.VMEM)
SMEM = pl.BlockSpec(memory_space=pltpu.SMEM)
HBM = pl.BlockSpec(memory_space=pltpu.HBM)
NN = (((1,), (0,)), ((), ()))
NT = (((1,), (1,)), ((), ()))


def dot(a, b, dims=NN):
    return lax.dot_general(a, b, dims, preferred_element_type=f32)


def halves(x):
    high = x.astype(bf16)
    return high, (x - high.astype(f32)).astype(bf16)


def dot3(ah, al, bh, bl, dims=NN):
    return dot(ah, bh, dims) + dot(ah, bl, dims) + dot(al, bh, dims)


def thirds(x):
    high = x.astype(bf16).astype(f32)
    rest = x - high
    mid = rest.astype(bf16).astype(f32)
    return jnp.concatenate([high, mid, rest - mid], axis=0).astype(bf16)


def one_hot(position, slots):
    rows = lax.broadcasted_iota(i32, (slots, position.shape[1]), 0)
    return jnp.where(rows == position, 1.0, 0.0).astype(bf16)


def span(index, size):
    return pl.ds(pl.multiple_of(index * size, size), size)


def pack_kernel(
    capacity, chunked, dest_ref, target_ref, weights_ref, corners_ref, velocity_hbm,
    out_ref, pos_ref, x0_ref, x1_ref, rows_ref, sem,
):
    owned = target_ref.shape[1]
    cells_x = velocity_hbm.shape[1]
    faces = [
        pltpu.make_async_copy(velocity_hbm.at[:, 0], x0_ref, sem.at[0]),
        pltpu.make_async_copy(velocity_hbm.at[:, cells_x - 1], x1_ref, sem.at[1]),
    ]
    for face in faces:
        face.start()
    dest = dest_ref[...]
    corner = corners_ref[0:1, :]
    lane = lax.broadcasted_iota(i32, (1, owned), 1)
    top = cells_x - SPAN
    last = corner > top // 2
    first = (dest * 2 + jnp.where(last, 1, 0)) * (cells_x * owned)
    key = first + jnp.where(last, top - corner, corner) * owned + lane
    column = jnp.transpose(jnp.broadcast_to(key, (8, owned)))[:, 0:1]
    ahead = jnp.where((column < key) & (column >= first), 1.0, 0.0)
    rank = jnp.sum(ahead, axis=0, keepdims=True).astype(i32)
    position = dest * capacity + jnp.where(last, capacity - 1 - rank, rank)
    pos_ref[...] = position
    rows_ref[0:3, :] = target_ref[...]
    for dim in range(3):
        rows_ref[3 + 6 * dim : 9 + 6 * dim, :] = weights_ref[dim]
    rows_ref[21:24, :] = corners_ref[...].astype(f32)
    slots = out_ref.size // ROWS
    moved = dot(thirds(rows_ref[...]), one_hot(position, slots), NT)
    moved = moved[0:ROWS] + moved[ROWS : 2 * ROWS] + moved[2 * ROWS :]
    if chunked:
        for chunk in range(slots // capacity):
            out_ref[chunk] = moved[:, chunk * capacity : (chunk + 1) * capacity]
    else:
        out_ref[...] = moved
    for face in faces:
        face.wait()


def window(weights, corner, length):
    offset = lax.broadcasted_iota(i32, (length, weights.shape[1]), 0) - corner
    out = jnp.zeros(offset.shape, f32)
    for k in range(SPAN):
        out = jnp.where(offset == k, weights[k : k + 1, :], out)
    return out


def tiles_of(arrived_ref, tile, slots):
    for t in range(slots // tile):
        at = slice(t * tile, (t + 1) * tile)
        if len(arrived_ref.shape) == 3:
            per = tile // arrived_ref.shape[2]
            yield at, jnp.concatenate([arrived_ref[t * per + k] for k in range(per)], axis=1)
        else:
            yield at, arrived_ref[:, at]


def quarter(chunk, chunks, capacity, index, width):
    lane = lax.broadcasted_iota(i32, (ROWS, capacity), 1)
    per = capacity // width
    out = []
    for base in range(0, chunks, per):
        piece = jnp.zeros((ROWS, capacity), f32)
        for k in range(per):
            moved = pltpu.roll(chunk(base + k), lax.rem(capacity + (k - index) * width, capacity), 1)
            piece = jnp.where((lane >= k * width) & (lane < (k + 1) * width), moved, piece)
        out.append(piece)
    return jnp.concatenate(out, axis=1)


def sample_kernel(
    tile, n_stream, quartered, band, arrived_ref, velocity_hbm,
    force_ref, wzh_hbm, wzl_hbm, wy_ref, fx_ref, y0_ref, y1_ref, start_ref,
    cell_ref, high_ref, low_ref, wzh_ref, wzl_ref, wx_ref, rel_ref, goal_ref, face_ref, in_sem, out_sem,
):
    cells_x, cells_z = y0_ref.shape[1:]
    cells_y, slots = wy_ref.shape
    pad = wx_ref.shape[0]
    count = slots // tile
    capacity = slots // n_stream
    width = tile // n_stream
    loads = [pltpu.make_async_copy(velocity_hbm.at[c], cell_ref.at[c], in_sem.at[c]) for c in range(3)]
    for load in loads:
        load.start()

    def tile_data(t):
        if quartered:
            return quarter(lambda k: arrived_ref[k], n_stream, capacity, t, width)
        if len(arrived_ref.shape) == 3:
            per = tile // capacity
            return jnp.concatenate([arrived_ref[t * per + k] for k in range(per)], axis=1)
        return arrived_ref[:, t * tile : (t + 1) * tile]

    kept = []
    fits = None
    for t in range(count):
        at = slice(t * tile, (t + 1) * tile)
        data = tile_data(t)
        corner = data[21:24, :].astype(i32)
        if quartered:
            used = data[3:4] != 0.0
            low = jnp.min(jnp.where(used, data[21:22], float(cells_x))).astype(i32)
            high = jnp.max(jnp.where(used, data[21:22], -1.0)).astype(i32)
            start = jnp.minimum(low, cells_x - band)
            inside = high + SPAN <= start + band
            fits = inside if fits is None else fits & inside
        else:
            start = 0
        kept.append((at, data, corner, start))
        wy_ref[:, at] = window(data[9:15], corner[1:2], cells_y)
        high, low = halves(window(data[15:21], corner[2:3], cells_z))
        wzh_ref[:, at] = high
        wzl_ref[:, at] = low
        for c in range(3):
            goal_ref[c, 0:1, at] = data[c : c + 1]
    stores = [
        pltpu.make_async_copy(wzh_ref, wzh_hbm, out_sem.at[0]),
        pltpu.make_async_copy(wzl_ref, wzl_hbm, out_sem.at[1]),
    ]
    for store in stores:
        store.start()
    if not quartered:
        fits = jnp.bool_(False)
    for t, (at, data, corner, start) in enumerate(kept):
        start = jnp.where(fits, start, 0)
        start_ref[t] = start
        wx_ref[:, at] = window(data[3:9], corner[0:1], pad)
        rel_ref[:, at] = window(data[3:9], corner[0:1] - start, pad)
    start_ref[count] = jnp.where(fits, 1, 0)
    for c in range(3):
        loads[c].wait()
        high, low = halves(cell_ref[c].reshape(cells_x * cells_y, cells_z))
        high_ref[c] = high
        low_ref[c] = low

    def sample(planes):
        def step(t, _):
            at = span(t, tile)
            rows = pl.ds(pl.multiple_of(start_ref[t] * cells_y, cells_y), planes * cells_y)
            wx = rel_ref[:, at]
            wy = wy_ref[:, at]
            for c in range(3):
                along = dot3(high_ref[c, rows, :], low_ref[c, rows, :], wzh_ref[:, at], wzl_ref[:, at])
                along = along.reshape(planes, cells_y, tile) * wy[None]
                sampled = jnp.sum(jnp.sum(along, axis=1) * wx[0:planes], axis=0, keepdims=True)
                force = goal_ref[c, 0:1, at] - sampled
                fx_ref[c, :, at] = force * wx
                goal_ref[c, 0:1, at] = force

        lax.fori_loop(0, count, step, None)

    if quartered:
        pl.when(fits)(lambda: sample(band))
        pl.when(jnp.logical_not(fits))(lambda: sample(cells_x))
    else:
        sample(cells_x)
    forces = [goal_ref[c, 0:1, :] for c in range(3)]
    if quartered:
        lane = lax.broadcasted_iota(i32, (8, capacity), 1)
        mixed = jnp.concatenate(forces + [jnp.zeros((5, slots), f32)], axis=0)
        per = capacity // width
        own = []
        for k in range(n_stream):
            piece = jnp.zeros((8, capacity), f32)
            for t in range(count):
                base = t * tile + k // per * capacity
                moved = pltpu.roll(mixed[:, base : base + capacity], (t - k % per) * width % capacity, 1)
                piece = jnp.where((lane >= t * width) & (lane < (t + 1) * width), moved, piece)
            own.append(piece)
        natural = jnp.concatenate(own, axis=1)[0:3]
    else:
        natural = jnp.concatenate(forces, axis=0)
    for k in range(force_ref.shape[0]):
        force_ref[k] = natural
    face_ref[...] = jnp.zeros_like(face_ref)

    def edges(t, _):
        at = span(t, tile)
        wx = wx_ref[:, at]
        wy = wy_ref[:, at]
        rows = [goal_ref[c, 0:1, at] * wx * wy[y : y + 1] for y in (0, cells_y - 1) for c in range(3)]
        high, low = halves(jnp.concatenate(rows, axis=0))
        face_ref[...] += dot3(high, low, wzh_ref[:, at], wzl_ref[:, at], NT)

    lax.fori_loop(0, count, edges, None)
    base = 0
    for y, ref in ((0, y0_ref), (cells_y - 1, y1_ref)):
        for c in range(3):
            ref[c] = cell_ref[c, :, y, :] + face_ref[base : base + cells_x]
            base += pad
    for store in stores:
        store.wait()


def spread_kernel(
    tile, quartered, band, velocity_hbm, wzh_ref, wzl_ref, wy_ref, fx_ref, start_ref, rhs_hbm, cell_ref, sum_ref, in_sem, out_sem,
):
    _, cells_x, cells_y, cells_z = velocity_hbm.shape
    count = wy_ref.shape[1] // tile
    loads = [pltpu.make_async_copy(velocity_hbm.at[c], cell_ref.at[c], in_sem.at[c]) for c in range(3)]
    stores = [pltpu.make_async_copy(cell_ref.at[c], rhs_hbm.at[c], out_sem.at[c]) for c in range(3)]
    for load in loads:
        load.start()
    sum_ref[...] = jnp.zeros_like(sum_ref)

    def spread(planes):
        def step(t, _):
            at = span(t, tile)
            rows = pl.ds(start_ref[t], planes)
            wy = wy_ref[:, at]
            for c in range(3):
                boxes = jnp.concatenate([fx_ref[c, x : x + 1, at] * wy for x in range(planes)], axis=0)
                high, low = halves(boxes)
                added = dot3(high, low, wzh_ref[:, at], wzl_ref[:, at], NT)
                sum_ref[c, rows] += added.reshape(planes, cells_y, cells_z)

        lax.fori_loop(0, count, step, None)

    if quartered:
        fits = start_ref[count] == 1
        pl.when(fits)(lambda: spread(band))
        pl.when(jnp.logical_not(fits))(lambda: spread(cells_x))
    else:
        spread(cells_x)
    for c in range(3):
        loads[c].wait()
        cell_ref[c] += sum_ref[c]
        stores[c].start()
    for store in stores:
        store.wait()


def finish_kernel(
    tile, n_stream, n_wall, chunked, quartered,
    rhs_hbm, x0_ref, x1_ref, y0_ref, y1_ref, left_ref, right_ref, given_ref, held_ref, pos_ref,
    next_hbm, force_ref, rhs_ref, next_ref, face_ref, marks_ref, in_sem, out_sem,
):
    _, cells_x, cells_y, cells_z = rhs_hbm.shape
    slots = given_ref.shape[2]
    loads = [pltpu.make_async_copy(rhs_hbm.at[c], rhs_ref.at[c], in_sem.at[c]) for c in range(3)]
    stores = [pltpu.make_async_copy(next_ref.at[c], next_hbm.at[c], out_sem.at[c]) for c in range(3)]
    for load in loads:
        load.start()
    here = lax.axis_index("gx")
    wall = lax.axis_index("gy")
    sides = (
        (0, left_ref, x0_ref, cells_x - SPAN, SPAN - 1, lax.rem(here + n_stream - 1, n_stream)),
        (1, right_ref, x1_ref, 0, 0, lax.rem(here + 1, n_stream)),
    )
    for side, arrived_ref, plane_ref, touching, row, owner in sides:
        face_ref[side] = plane_ref[...]

        def add(data, force):
            corner = data[21:24, :].astype(i32)
            wy = window(data[9:15], corner[1:2], cells_y)
            wzh, wzl = halves(window(data[15:21], corner[2:3], cells_z))
            wx = jnp.where(corner[0:1] == touching, data[3 + row : 4 + row], 0.0)
            force = force * wx
            high, low = halves(jnp.concatenate([force[c : c + 1] * wy for c in range(3)], axis=0))
            face_ref[side] += dot3(high, low, wzh, wzl, NT).reshape(3, cells_y, cells_z)

        if quartered:
            capacity = slots // n_stream
            width = tile // n_stream
            for k in range(n_stream):
                marks_ref[side, k] = arrived_ref[k]
                marks_ref[side, k, 0:3] = given_ref[owner, :, k * capacity : (k + 1) * capacity]
            held = marks_ref[side]
            touches = (held[:, 21, :] == float(touching)) & (held[:, 3, :] != 0.0)
            lane = lax.broadcasted_iota(i32, touches.shape, 1)
            depth = lane + 1 if side else capacity - lane
            reach = jnp.max(jnp.where(touches, depth.astype(f32), 0.0)).astype(i32)
            per = capacity // width

            def step(index, _):
                at = index if side else per - 1 - index
                data = quarter(lambda k: marks_ref[side, k], n_stream, capacity, at, width)
                add(data, data[0:3])

            lax.fori_loop(0, lax.div(reach + width - 1, width), step, None)
        else:
            for at, data in tiles_of(arrived_ref, tile, slots):
                add(data, given_ref[owner, :, at])
    y = lax.broadcasted_iota(i32, (cells_y, cells_z), 0)
    lower = jnp.where(wall == 0, 0.0, 1.0).astype(f32)
    upper = jnp.where(wall == n_wall - 1, 0.0, 1.0).astype(f32)
    scale = 1.0 / (1.0 + 6.0 * diffusion)
    for c in range(3):
        loads[c].wait()
        for x in range(cells_x):
            cell = rhs_ref[c, x]
            back = rhs_ref[c, x - 1] if x else face_ref[0, c]
            ahead = rhs_ref[c, x + 1] if x < cells_x - 1 else face_ref[1, c]
            below = jnp.where(y == 0, y0_ref[c, x : x + 1, :] * lower, pltpu.roll(cell, 1, 0))
            above = jnp.where(y == cells_y - 1, y1_ref[c, x : x + 1, :] * upper, pltpu.roll(cell, cells_y - 1, 0))
            side = pltpu.roll(cell, 1, 1) + pltpu.roll(cell, cells_z - 1, 1)
            near = (ahead + back) + (above + below) + side
            next_ref[c, x] = (cell + diffusion * near) * scale
        stores[c].start()
    if chunked:
        capacity = slots // n_stream
        mine = span(here, capacity)
        held = jnp.concatenate([given_ref[k, :, mine] for k in range(n_stream)], axis=1)
    else:
        held = held_ref[...]
    held = jnp.concatenate([held, jnp.zeros((5, slots), f32)], axis=0)
    moved = dot(thirds(held), one_hot(pos_ref[...], slots))
    moved = moved[0:8] + moved[8:16] + moved[16:24]
    force_ref[...] = moved[0:3]
    for store in stores:
        store.wait()


def per_device(velocity, target, weights, corners, dest):
    n_stream = lax.axis_size("gx")
    n_wall = lax.axis_size("gy")
    owned = target.shape[1]
    capacity = max(SLOT_MIN, 2 * owned // n_stream)
    slots = n_stream * capacity
    _, cells_x, cells_y, cells_z = velocity.shape
    block = cells_x * cells_y
    chunked = capacity % 128 == 0
    tile = 256 if slots % 256 == 0 else 128
    quartered = capacity == 128 and tile % n_stream == 0 and capacity % (tile // n_stream) == 0
    band = min(cells_x, SPAN + (cells_x - SPAN + 1) // 2)
    shape = jax.ShapeDtypeStruct
    sems = pltpu.SemaphoreType.DMA

    face_x = shape((3, cells_y, cells_z), f32)
    outgoing, position, x0, x1 = pl.pallas_call(
        functools.partial(pack_kernel, capacity, chunked),
        out_shape=(
            shape((n_stream, ROWS, capacity) if chunked else (ROWS, slots), f32),
            shape((1, owned), i32),
            face_x,
            face_x,
        ),
        in_specs=[VMEM] * 4 + [HBM],
        out_specs=(VMEM,) * 4,
        scratch_shapes=[pltpu.VMEM((ROWS, owned), f32), sems((2,))],
        name="pack",
    )(dest.reshape(1, owned), target, weights, corners, velocity)
    if chunked:
        arrived = lax.all_to_all(outgoing, "gx", split_axis=0, concat_axis=0, tiled=True)
    else:
        outgoing = outgoing.reshape(ROWS, n_stream, capacity)
        arrived = lax.all_to_all(outgoing, "gx", split_axis=1, concat_axis=1, tiled=True)
        arrived = arrived.reshape(ROWS, slots)

    up_x = [(i, (i + 1) % n_stream) for i in range(n_stream)]
    down_x = [(j, i) for i, j in up_x]
    up_y = [(i, (i + 1) % n_wall) for i in range(n_wall)]
    down_y = [(j, i) for i, j in up_y]
    from_x0 = lax.ppermute(x1, "gx", up_x)
    from_x1 = lax.ppermute(x0, "gx", down_x)
    left = lax.ppermute(arrived, "gx", up_x)
    right = lax.ppermute(arrived, "gx", down_x)

    pad = -(-cells_x // 16) * 16
    force, wzh, wzl, wy, fx, y0, y1, starts = pl.pallas_call(
        functools.partial(sample_kernel, tile, n_stream, quartered, band),
        out_shape=(
            shape((n_stream, 3, slots), f32),
            shape((cells_z, slots), bf16),
            shape((cells_z, slots), bf16),
            shape((cells_y, slots), f32),
            shape((3, pad, slots), f32),
            shape((3, cells_x, cells_z), f32),
            shape((3, cells_x, cells_z), f32),
            shape((slots // tile + 1,), i32),
        ),
        in_specs=[VMEM, HBM],
        out_specs=(VMEM, HBM, HBM, VMEM, VMEM, VMEM, VMEM, SMEM),
        scratch_shapes=[
            pltpu.VMEM(velocity.shape, f32),
            pltpu.VMEM((3, block, cells_z), bf16),
            pltpu.VMEM((3, block, cells_z), bf16),
            pltpu.VMEM((cells_z, slots), bf16),
            pltpu.VMEM((cells_z, slots), bf16),
            pltpu.VMEM((pad, slots), f32),
            pltpu.VMEM((pad, slots), f32),
            pltpu.VMEM((3, 8, slots), f32),
            pltpu.VMEM((6 * pad, cells_z), f32),
            sems((3,)),
            sems((2,)),
        ],
        compiler_params=pltpu.CompilerParams(vmem_limit_bytes=63_280_000),
        name="sample",
    )(arrived, velocity)

    from_y0 = lax.ppermute(y1, "gy", up_y)
    from_y1 = lax.ppermute(y0, "gy", down_y)
    given = lax.all_to_all(force, "gx", split_axis=0, concat_axis=0, tiled=True)
    if chunked:
        held = position
    else:
        held = lax.dynamic_slice_in_dim(given, lax.axis_index("gx") * capacity, capacity, axis=2)
        held = held.transpose(1, 0, 2).reshape(3, slots)

    rhs = pl.pallas_call(
        functools.partial(spread_kernel, tile, quartered, band),
        out_shape=shape(velocity.shape, f32),
        in_specs=[HBM, VMEM, VMEM, VMEM, VMEM, SMEM],
        out_specs=HBM,
        scratch_shapes=[
            pltpu.VMEM(velocity.shape, f32),
            pltpu.VMEM(velocity.shape, f32),
            sems((3,)),
            sems((3,)),
        ],
        cost_estimate=pl.CostEstimate(flops=18 * block * slots * cells_z, bytes_accessed=24 * block * cells_z, transcendentals=0),
        name="spread",
    )(velocity, wzh, wzl, wy, fx, starts)

    return pl.pallas_call(
        functools.partial(finish_kernel, tile, n_stream, n_wall, chunked, quartered),
        out_shape=(shape(velocity.shape, f32), shape((3, owned), f32)),
        in_specs=[HBM] + [VMEM] * 9,
        out_specs=(HBM, VMEM),
        scratch_shapes=[
            pltpu.VMEM(velocity.shape, f32),
            pltpu.VMEM(velocity.shape, f32),
            pltpu.VMEM((2, 3, cells_y, cells_z), f32),
            pltpu.VMEM((2, n_stream, ROWS, 128), f32),
            sems((3,)),
            sems((3,)),
        ],
        compiler_params=pltpu.CompilerParams(vmem_limit_bytes=62_400_000),
        name="finish",
    )(rhs, from_x0, from_x1, from_y0, from_y1, left, right, given, held, position)


def solution(mesh):
    in_specs = (
        P(None, "gx", "gy", None),
        P(None, ("gx", "gy")),
        P(None, None, ("gx", "gy")),
        P(None, ("gx", "gy")),
        P(("gx", "gy"), None),
    )
    out_specs = (P(None, "gx", "gy", None), P(None, ("gx", "gy")))
    return jax.shard_map(
        per_device, mesh=mesh, in_specs=in_specs, out_specs=out_specs, check_vma=False
    )
```
